8 devices in a mesh: dp: 1 (over z), pp: 8 (over y, x, core).
Axes of the slice: x: 2, y: 2, z: 1, core: 2. Of those that a mesh axis runs over, the one named last changes fastest.
Arguments:
- acts_in: bfloat16 [8, 2, 512, 1536], P(None, 'dp')
- cotangent: bfloat16 [8, 2, 512, 1536], P(None, 'dp')
- ln1_gain: bfloat16 [8, 1536], P('pp')
- ln1_shift: bfloat16 [8, 1536], P('pp')
- w_qkv: bfloat16 [8, 1536, 4608], P('pp')
- b_qkv: bfloat16 [8, 4608], P('pp')
- w_proj: bfloat16 [8, 16, 96, 1536], P('pp')
- b_proj: bfloat16 [8, 1536], P('pp')
- ln2_gain: bfloat16 [8, 1536], P('pp')
- ln2_shift: bfloat16 [8, 1536], P('pp')
- w_up: bfloat16 [8, 1536, 6144], P('pp')
- b_up: bfloat16 [8, 6144], P('pp')
- w_down: bfloat16 [8, 6144, 1536], P('pp')
- b_down: bfloat16 [8, 1536], P('pp')
Outputs:
- output 1: bfloat16 [8, 2, 512, 1536], P(None, 'dp')
- output 2: bfloat16 [8, 2, 512, 1536], P(None, 'dp')
- output 3: float32 [8, 1536], P(('dp', 'pp'))
- output 4: float32 [8, 1536], P(('dp', 'pp'))
- output 5: float32 [8, 1536, 4608], P(('dp', 'pp'))
- output 6: float32 [8, 4608], P(('dp', 'pp'))
- output 7: float32 [8, 16, 96, 1536], P(('dp', 'pp'))
- output 8: float32 [8, 1536], P(('dp', 'pp'))
- output 9: float32 [8, 1536], P(('dp', 'pp'))
- output 10: float32 [8, 1536], P(('dp', 'pp'))
- output 11: float32 [8, 1536, 6144], P(('dp', 'pp'))
- output 12: float32 [8, 6144], P(('dp', 'pp'))
- output 13: float32 [8, 6144, 1536], P(('dp', 'pp'))
- output 14: float32 [8, 1536], P(('dp', 'pp'))
All inputs are finite; a program needn't handle non-finite values.
Results may differ from the reference program's by a relative error of at most 0.02.
Values are sent between devices in bfloat16 or wider.
A program may use at most 1.25 GiB of HBM per device.

```python
import jax
import jax.numpy as jnp
from jax import lax

D = 1536
HEADS = 16
LAYERS = 8
MICRO = 8
BATCH = 2
SEQ = 512
HEAD = D // HEADS
TOKENS = BATCH * SEQ
LN_EPS = 1e-5


def setup_inputs(seed: int = 0, part: int = 0) -> dict:
    part_key = jax.random.fold_in(jax.random.key(seed), part)
    key_x, key_ct = jax.random.split(part_key)
    key_list = jax.random.split(jax.random.key(seed + 1), 12)
    act_shape = (MICRO, BATCH, SEQ, D)

    def draw_normal(rng_key, arr_dims, scale_by):
        return jax.random.normal(rng_key, arr_dims, jnp.float32) * scale_by

    return {
        'acts_in': draw_normal(key_x, act_shape, 1.0).astype(jnp.bfloat16),
        'cotangent': draw_normal(key_ct, act_shape, 1.0).astype(jnp.bfloat16),
        'ln1_gain': (1.0 + draw_normal(key_list[0], (LAYERS, D), 0.2)).astype(jnp.bfloat16),
        'ln1_shift': draw_normal(key_list[1], (LAYERS, D), 0.3).astype(jnp.bfloat16),
        'w_qkv': draw_normal(key_list[2], (LAYERS, D, 3 * D), D ** -0.5).astype(jnp.bfloat16),
        'b_qkv': draw_normal(key_list[3], (LAYERS, 3 * D), 0.3).astype(jnp.bfloat16),
        'w_proj': draw_normal(key_list[4], (LAYERS, HEADS, HEAD, D), D ** -0.5).astype(jnp.bfloat16),
        'b_proj': draw_normal(key_list[5], (LAYERS, D), 0.3).astype(jnp.bfloat16),
        'ln2_gain': (1.0 + draw_normal(key_list[6], (LAYERS, D), 0.2)).astype(jnp.bfloat16),
        'ln2_shift': draw_normal(key_list[7], (LAYERS, D), 0.3).astype(jnp.bfloat16),
        'w_up': draw_normal(key_list[8], (LAYERS, D, 4 * D), D ** -0.5).astype(jnp.bfloat16),
        'b_up': draw_normal(key_list[9], (LAYERS, 4 * D), 0.3).astype(jnp.bfloat16),
        'w_down': draw_normal(key_list[10], (LAYERS, 4 * D, D), (4 * D) ** -0.5).astype(jnp.bfloat16),
        'b_down': draw_normal(key_list[11], (LAYERS, D), 0.3).astype(jnp.bfloat16),
    }


def layer_norm(x_wide, gain, shift):
    mean_val = jnp.mean(x_wide, axis=-1, keepdims=True)
    centered = x_wide - mean_val
    variance = jnp.mean(centered * centered, axis=-1, keepdims=True)
    return centered * lax.rsqrt(variance + LN_EPS) * gain + shift


def mat_mul(act_rows, weight):
    return jnp.dot(act_rows.astype(jnp.float32), weight, preferred_element_type=jnp.float32)


def layer_forward(weights, x_act):
    g_one, s_one, w_qkv, b_qkv, w_proj, b_proj, g_two, s_two, w_up, b_up, w_down, b_down = weights
    x_wide = x_act.astype(jnp.float32)
    h_one = layer_norm(x_wide, g_one, s_one).astype(jnp.bfloat16)
    qkv_act = (mat_mul(h_one, w_qkv) + b_qkv).astype(jnp.bfloat16)
    qkv_heads = qkv_act.astype(jnp.float32).reshape(BATCH, SEQ, 3, HEADS, HEAD)
    scores = jnp.einsum('bqhd,bkhd->bhqk', qkv_heads[:, :, 0], qkv_heads[:, :, 1]) * (HEAD ** -0.5)
    causal = jnp.arange(SEQ)[:, None] >= jnp.arange(SEQ)[None, :]
    attn_probs = jax.nn.softmax(jnp.where(causal, scores, -1e30), axis=-1).astype(jnp.bfloat16)
    attn_mix = jnp.einsum('bhqk,bkhd->bqhd', attn_probs.astype(jnp.float32), qkv_heads[:, :, 2]).astype(jnp.bfloat16)
    x_mid = (x_wide + mat_mul(attn_mix.reshape(TOKENS, D), w_proj.reshape(D, D)) + b_proj).astype(jnp.bfloat16)
    mid_wide = x_mid.astype(jnp.float32)
    h_two = layer_norm(mid_wide, g_two, s_two).astype(jnp.bfloat16)
    hidden = jax.nn.gelu(mat_mul(h_two, w_up) + b_up, approximate=True).astype(jnp.bfloat16)
    return (mid_wide + mat_mul(hidden, w_down) + b_down).astype(jnp.bfloat16)


def reference(acts_in, cotangent, ln1_gain, ln1_shift, w_qkv, b_qkv, w_proj, b_proj, ln2_gain, ln2_shift, w_up, b_up, w_down, b_down):
    weights = tuple(tensor.astype(jnp.float32) for tensor in (ln1_gain, ln1_shift, w_qkv, b_qkv, w_proj, b_proj, ln2_gain, ln2_shift, w_up, b_up, w_down, b_down))

    def stack_forward(stack_w, x_act):
        def layer_step(carry_act, layer_w):
            return layer_forward(layer_w, carry_act), None
        final_act, unused = lax.scan(layer_step, x_act, stack_w)
        return final_act

    def micro_step(grad_acc, mb_pair):
        x_mb, ct_mb = mb_pair
        y_rows, pull_back = jax.vjp(stack_forward, weights, x_mb.reshape(TOKENS, D))
        w_grads, x_grad = pull_back(ct_mb.reshape(TOKENS, D))
        new_acc = tuple(acc_old + new_grad for acc_old, new_grad in zip(grad_acc, w_grads))
        return new_acc, (y_rows.reshape(BATCH, SEQ, D), x_grad.reshape(BATCH, SEQ, D))

    zero_acc = tuple(jnp.zeros_like(tensor) for tensor in weights)
    grad_sums, (acts_out, grad_in) = lax.scan(micro_step, zero_acc, (acts_in, cotangent))
    return (acts_out, grad_in, grad_sums[0], grad_sums[1], grad_sums[2], grad_sums[3], grad_sums[4], grad_sums[5], grad_sums[6], grad_sums[7], grad_sums[8], grad_sums[9], grad_sums[10], grad_sums[11])
```

```python
import functools
import jax
import jax.numpy as jnp
from jax import lax
from jax.experimental import pallas as pl
from jax.experimental.pallas import tpu as pltpu
from jax.sharding import PartitionSpec as P

LN_EPS = 1e-5
PARAM_RANKS = (2, 2, 3, 2, 4, 2, 2, 2, 3, 2, 3, 2)
BF, F32 = jnp.bfloat16, jnp.float32
LOG2E = 1.4426950408889634
GC0 = 0.7978845608028654
GC1 = GC0 * 0.044715
NT = (((1,), (1,)), ((), ()))
NN = (((1,), (0,)), ((), ()))
TN = (((0,), (0,)), ((), ()))


def mm(a, b, dims=NN):
    return lax.dot_general(a, b, dims, preferred_element_type=F32)


def ln_stats(x_wide):
    mean_val = jnp.mean(x_wide, axis=-1, keepdims=True)
    centered = x_wide - mean_val
    variance = jnp.mean(centered * centered, axis=-1, keepdims=True)
    rstd = lax.rsqrt(variance + LN_EPS)
    return centered * rstd, rstd


def ln_back(dh, xhat, rstd, gain):
    dxh = dh * gain
    c1 = jnp.mean(dxh, axis=-1, keepdims=True)
    c2 = jnp.mean(dxh * xhat, axis=-1, keepdims=True)
    return rstd * (dxh - c1 - xhat * c2)


HEAD_WIN = ((0, 128), (0, 256), (128, 384), (256, 384))


def head_mask(j):
    lo, hi = HEAD_WIN[j]
    lane = lax.broadcasted_iota(jnp.int32, (1, hi - lo), 1) + lo
    keep = (lane >= 96 * j) & (lane < 96 * j + 96)
    return jnp.where(keep, 1.0, 0.0).astype(BF)


def fwd_kernel(n_qkv, n_grp, n_proj, n_mlp, idx, x_ref, g1, s1, wqkv, bqkv, wproj, bproj, g2, s2, wup, bup, wdown, bdown,
               _a0, _a1, _a2, _a3, _a4, _a5, _a6,
               y_ref, xs_ref, h1_ref, qkv_ref, mix_ref, x1_ref, h2_ref, pre_ref,
               qkv_s, mix_s, h_s, act_s, acc_s):
    step = pl.program_id(0)
    b0, b1, b2 = n_qkv, n_qkv + n_grp, n_qkv + n_grp + n_proj
    tq, tp, tf = wqkv.shape[1], wproj.shape[1], wup.shape[1]
    d = x_ref.shape[1]
    n_seq = x_ref.shape[0]
    half = n_seq // 2

    @pl.when(step == 0)
    def _():
        x = x_ref[...]
        xs_ref[0] = x
        xhat, _ = ln_stats(x.astype(F32))
        h = (xhat * g1[...].astype(F32) + s1[...].astype(F32)).astype(BF)
        h_s[...] = h
        h1_ref[0] = h

    @pl.when(step < b0)
    def _():
        t = (mm(h_s[...], wqkv[...]) + bqkv[...].astype(F32)).astype(BF)
        qkv_ref[0] = t
        qkv_s[:, pl.ds(pl.multiple_of(step * tq, 128), tq)] = t

    @pl.when((step >= b0) & (step < b1))
    def _():
        grp = step - b0
        sl = lambda p: pl.ds(pl.multiple_of(p * d + grp * 384, 128), 384)
        q, k, v = qkv_s[:, sl(0)], qkv_s[:, sl(1)], qkv_s[:, sl(2)]
        rows = lax.broadcasted_iota(jnp.int32, (half, half), 0)
        cols = lax.broadcasted_iota(jnp.int32, (half, half), 1)
        causal = rows >= cols
        sc = (96.0 ** -0.5) * LOG2E
        outs = []
        for j in range(4):
            lo, hi = HEAD_WIN[j]
            m = head_mask(j)
            qm, vm, kw = q[:, lo:hi] * m, v[:, lo:hi] * m, k[:, lo:hi]
            s00 = jnp.where(causal, mm(qm[:half], kw[:half], NT), -1e30)
            s10 = mm(qm[half:], kw[:half], NT)
            s11 = jnp.where(causal, mm(qm[half:], kw[half:], NT), -1e30)
            m0 = jnp.max(s00, axis=1, keepdims=True)
            e00 = jnp.exp2((s00 - m0) * sc)
            p00 = (e00 * (1.0 / jnp.sum(e00, axis=1, keepdims=True))).astype(BF)
            o0 = mm(p00, vm[:half])
            m1 = jnp.maximum(jnp.max(s10, axis=1, keepdims=True), jnp.max(s11, axis=1, keepdims=True))
            e10 = jnp.exp2((s10 - m1) * sc)
            e11 = jnp.exp2((s11 - m1) * sc)
            r1 = 1.0 / (jnp.sum(e10, axis=1, keepdims=True) + jnp.sum(e11, axis=1, keepdims=True))
            p10 = (e10 * r1).astype(BF)
            p11 = (e11 * r1).astype(BF)
            o1 = mm(p10, vm[:half]) + mm(p11, vm[half:])
            outs.append(jnp.concatenate([o0, o1], axis=0))
        t0 = outs[0] + outs[1][:, :128]
        t1 = outs[1][:, 128:] + outs[2][:, :128]
        t2 = outs[2][:, 128:] + outs[3]
        o = jnp.concatenate([t0, t1, t2], axis=1).astype(BF)
        mix_ref[0] = o
        mix_s[:, pl.ds(pl.multiple_of(grp * 384, 128), 384)] = o

    @pl.when((step >= b1) & (step < b2))
    def _():
        c = pl.ds(pl.multiple_of((step - b1) * tp, 128), tp)
        acc_s[:, c] = mm(mix_s[...], wproj[...]) + bproj[...].astype(F32)

    @pl.when(step == b2 - 1)
    def _():
        x1 = (x_ref[...].astype(F32) + acc_s[...]).astype(BF)
        x1_ref[0] = x1
        x1w = x1.astype(F32)
        xhat, _ = ln_stats(x1w)
        h = (xhat * g2[...].astype(F32) + s2[...].astype(F32)).astype(BF)
        h_s[...] = h
        h2_ref[0] = h
        acc_s[...] = x1w + bdown[...].astype(F32)

    def up():
        pre = mm(h_s[...], wup[...]) + bup[...].astype(F32)
        pre_ref[0] = pre
        t = jnp.tanh(pre * (GC0 + GC1 * (pre * pre)))
        return (0.5 * pre * (1.0 + t)).astype(BF)

    @pl.when(step == b2)
    def _():
        act_s[0] = up()

    @pl.when((step > b2) & (step < b2 + n_mlp))
    def _():
        slot = lax.rem(step - b2, 2)
        act_s[slot] = up()
        acc_s[...] += mm(act_s[1 - slot], wdown[...])

    @pl.when(step == b2 + n_mlp)
    def _():
        y_ref[...] = (acc_s[...] + mm(act_s[1 - lax.rem(step - b2, 2)], wdown[...])).astype(BF)


def fwd_call(idx, x, weights, saved):
    g1, s1, wqkv, bqkv, wproj, bproj, g2, s2, wup, bup, wdown, bdown = weights
    n_seq, d = x.shape
    e, f = wqkv.shape[1], wup.shape[1]
    tq, tp, tf = 768, 768, 512
    n_qkv, n_grp, n_proj, n_mlp = e // tq, 4, d // tp, f // tf
    b0, b1, b2 = n_qkv, n_qkv + n_grp, n_qkv + n_grp + n_proj
    full = lambda i, ix: (0, 0)
    row3 = lambda i, ix: (ix[0], 0, 0)
    cq = lambda i, ix: (0, jnp.clip(i, 0, n_qkv - 1))
    cp = lambda i, ix: (0, jnp.clip(i - b1, 0, n_proj - 1))
    cu = lambda i, ix: (0, jnp.clip(i - b2, 0, n_mlp - 1))
    rd = lambda i, ix: (jnp.clip(i - b2 - 1, 0, n_mlp - 1), 0)
    any_spec = pl.BlockSpec(memory_space=pl.ANY)
    in_specs = [
        pl.BlockSpec((n_seq, d), full), pl.BlockSpec((1, d), full), pl.BlockSpec((1, d), full),
        pl.BlockSpec((d, tq), cq), pl.BlockSpec((1, tq), cq),
        pl.BlockSpec((d, tp), cp), pl.BlockSpec((1, tp), cp),
        pl.BlockSpec((1, d), full), pl.BlockSpec((1, d), full),
        pl.BlockSpec((d, tf), cu), pl.BlockSpec((1, tf), cu),
        pl.BlockSpec((tf, d), rd), pl.BlockSpec((1, d), full),
    ] + [any_spec] * 7
    out_specs = [
        pl.BlockSpec((n_seq, d), full),
        pl.BlockSpec((1, n_seq, d), row3),
        pl.BlockSpec((1, n_seq, d), row3),
        pl.BlockSpec((1, n_seq, tq), lambda i, ix: (ix[0], 0, jnp.clip(i, 0, n_qkv - 1))),
        pl.BlockSpec((1, n_seq, 384), lambda i, ix: (ix[0], 0, jnp.clip(i - b0, 0, n_grp - 1))),
        pl.BlockSpec((1, n_seq, d), row3),
        pl.BlockSpec((1, n_seq, d), row3),
        pl.BlockSpec((1, n_seq, tf), lambda i, ix: (ix[0], 0, jnp.clip(i - b2, 0, n_mlp - 1))),
    ]
    r2 = lambda t: t.reshape(1, -1)
    args = [idx, x, r2(g1), r2(s1), wqkv, r2(bqkv), wproj.reshape(d, d), r2(bproj), r2(g2), r2(s2), wup, r2(bup), wdown, r2(bdown)]
    outs = pl.pallas_call(
        functools.partial(fwd_kernel, n_qkv, n_grp, n_proj, n_mlp),
        grid_spec=pltpu.PrefetchScalarGridSpec(
            num_scalar_prefetch=1, grid=(b2 + n_mlp + 1,), in_specs=in_specs, out_specs=out_specs,
            scratch_shapes=[pltpu.VMEM((n_seq, e), BF), pltpu.VMEM((n_seq, d), BF), pltpu.VMEM((n_seq, d), BF),
                            pltpu.VMEM((2, n_seq, tf), BF), pltpu.VMEM((n_seq, d), F32)]),
        out_shape=[jax.ShapeDtypeStruct((n_seq, d), BF)] + [jax.ShapeDtypeStruct(s.shape, s.dtype) for s in saved],
        input_output_aliases={14 + i: 1 + i for i in range(7)},
        compiler_params=pltpu.CompilerParams(dimension_semantics=("arbitrary",), vmem_limit_bytes=60 * 1024 * 1024),
        cost_estimate=pl.CostEstimate(flops=int(31e9), bytes_accessed=int(9e7), transcendentals=0),
        name="layer_fwd",
    )(*args, *saved)
    return outs[0], tuple(outs[1:])


def bwd_kernel(n_mlp, n_proj, n_grp, n_qkv, idx, dy_ref, pre_ref, x1_ref, q_ref, k_ref, v_ref, x_ref,
               wdown, wup, wproj, wqkv, g1, g2,
               _a0, _a1, _a2, _a3, _a4, _a5, _a6, _a7,
               dx_ref, act_ref, dpre_ref, dmid_ref, dqkv_ref, dys_ref, sup_ref, sqkv_ref, sd_ref,
               acc_s, dp_s, dm_s, do_s, dqkv_s):
    step = pl.program_id(0)
    b0 = n_mlp + 1
    b1, b2 = b0 + n_proj, b0 + n_proj + n_grp
    d = dy_ref.shape[1]
    n_seq = dy_ref.shape[0]
    half = n_seq // 2
    tp, tq = wproj.shape[0], wqkv.shape[1]
    colsum = lambda t: jnp.sum(t, axis=0, keepdims=True)

    def down_back():
        da = mm(dy_ref[...], wdown[...], NT).astype(BF).astype(F32)
        pre = pre_ref[0]
        p2 = pre * pre
        t = jnp.tanh(pre * (GC0 + GC1 * p2))
        u = 0.5 * (1.0 + t)
        act_ref[0] = (pre * u).astype(BF)
        dpre = da * (u + 0.5 * pre * (1.0 - t * t) * (GC0 + 3.0 * GC1 * p2))
        sup_ref[0] = colsum(dpre)
        dpb = dpre.astype(BF)
        dpre_ref[0] = dpb
        return dpb

    @pl.when(step == 0)
    def _():
        dy = dy_ref[...]
        dys_ref[0] = dy
        sd_ref[0, 5:6, :] = colsum(dy.astype(F32))
        acc_s[...] = jnp.zeros_like(acc_s)
        dp_s[0] = down_back()

    @pl.when((step > 0) & (step < n_mlp))
    def _():
        slot = lax.rem(step, 2)
        dp_s[slot] = down_back()
        acc_s[...] += mm(dp_s[1 - slot], wup[...], NT)

    @pl.when(step == n_mlp)
    def _():
        dh = (acc_s[...] + mm(dp_s[1 - lax.rem(step, 2)], wup[...], NT)).astype(BF).astype(F32)
        xhat, rstd = ln_stats(x1_ref[0].astype(F32))
        sd_ref[0, 2:3, :] = colsum(dh * xhat)
        sd_ref[0, 3:4, :] = colsum(dh)
        dm = (dy_ref[...].astype(F32) + ln_back(dh, xhat, rstd, g2[...].astype(F32))).astype(BF)
        dm_s[...] = dm
        dmid_ref[0] = dm
        sd_ref[0, 4:5, :] = colsum(dm.astype(F32))

    @pl.when((step >= b0) & (step < b1))
    def _():
        c = pl.ds(pl.multiple_of((step - b0) * tp, 128), tp)
        do_s[:, c] = mm(dm_s[...], wproj[...], NT).astype(BF)

    @pl.when((step >= b1) & (step < b2))
    def _():
        grp = step - b1
        q, k, v = q_ref[0], k_ref[0], v_ref[0]
        do = do_s[:, pl.ds(pl.multiple_of(grp * 384, 128), 384)]
        keys = lax.broadcasted_iota(jnp.int32, (half, n_seq), 0)
        qrys = lax.broadcasted_iota(jnp.int32, (half, n_seq), 1)
        ok0 = keys <= qrys
        ok1 = ok0[:, :half]
        scale = 96.0 ** -0.5
        sc = scale * LOG2E
        dqs, dks, dvs = [], [], []
        for j in range(4):
            lo, hi = HEAD_WIN[j]
            m = head_mask(j)
            qm, km, dom = q[:, lo:hi] * m, k[:, lo:hi] * m, do[:, lo:hi] * m
            kw, vw = k[:, lo:hi], v[:, lo:hi]
            st0 = jnp.where(ok0, mm(kw[:half], qm, NT), -1e30)
            st1 = jnp.where(ok1, mm(kw[half:], qm[half:], NT), -1e30)
            mx = jnp.max(st0, axis=0, keepdims=True)
            mr = jnp.maximum(mx[:, half:], jnp.max(st1, axis=0, keepdims=True))
            mx = jnp.concatenate([mx[:, :half], mr], axis=1)
            e0 = jnp.exp2((st0 - mx) * sc)
            e1 = jnp.exp2((st1 - mr) * sc)
            l0 = jnp.sum(e0, axis=0, keepdims=True)
            lr = l0[:, half:] + jnp.sum(e1, axis=0, keepdims=True)
            inv = 1.0 / jnp.concatenate([l0[:, :half], lr], axis=1)
            p0 = e0 * inv
            p1 = e1 * inv[:, half:]
            dp0 = mm(vw[:half], dom, NT).astype(BF).astype(F32)
            dp1 = mm(vw[half:], dom[half:], NT).astype(BF).astype(F32)
            rd = jnp.sum(p0 * dp0, axis=0, keepdims=True)
            rr = rd[:, half:] + jnp.sum(p1 * dp1, axis=0, keepdims=True)
            rd = jnp.concatenate([rd[:, :half], rr], axis=1)
            ds0 = (p0 * (dp0 - rd) * scale).astype(BF)
            ds1 = (p1 * (dp1 - rr) * scale).astype(BF)
            p0b, p1b = p0.astype(BF), p1.astype(BF)
            dvs.append(jnp.concatenate([mm(p0b, dom), mm(p1b, dom[half:])], axis=0))
            dks.append(jnp.concatenate([mm(ds0, qm), mm(ds1, qm[half:])], axis=0))
            dq0 = mm(ds0[:, :half], km[:half], TN)
            dq1 = mm(jnp.concatenate([ds0[:, half:], ds1], axis=0), km, TN)
            dqs.append(jnp.concatenate([dq0, dq1], axis=0))
        for part, t in enumerate((dqs, dks, dvs)):
            g = jnp.concatenate([t[0] + t[1][:, :128], t[1][:, 128:] + t[2][:, :128], t[2][:, 128:] + t[3]], axis=1).astype(BF)
            dqkv_s[:, pl.ds(pl.multiple_of(part * d + grp * 384, 128), 384)] = g

    @pl.when(step == b2)
    def _():
        acc_s[...] = jnp.zeros_like(acc_s)

    @pl.when(step >= b2)
    def _():
        t = dqkv_s[:, pl.ds(pl.multiple_of((step - b2) * tq, 128), tq)]
        dqkv_ref[0] = t
        sqkv_ref[0] = colsum(t.astype(F32))
        acc_s[...] += mm(t, wqkv[...], NT)

    @pl.when(step == b2 + n_qkv - 1)
    def _():
        dh = acc_s[...].astype(BF).astype(F32)
        xhat, rstd = ln_stats(x_ref[0].astype(F32))
        sd_ref[0, 0:1, :] = colsum(dh * xhat)
        sd_ref[0, 1:2, :] = colsum(dh)
        dx_ref[...] = (dm_s[...].astype(F32) + ln_back(dh, xhat, rstd, g1[...].astype(F32))).astype(BF)


def bwd_call(idx, dy, weights, saved, store):
    g1, s1, wqkv, bqkv, wproj, bproj, g2, s2, wup, bup, wdown, bdown = weights
    xs, h1, qkv, mix, x1, h2, pre = saved
    n_seq, d = dy.shape
    e, f = wqkv.shape[1], wup.shape[1]
    tq, tp, tf = 768, 768, 512
    n_qkv, n_grp, n_proj, n_mlp = e // tq, 4, d // tp, f // tf
    b0 = n_mlp + 1
    b1, b2 = b0 + n_proj, b0 + n_proj + n_grp
    full = lambda i, ix: (0, 0)
    row3 = lambda i, ix: (ix[0], 0, 0)
    mlp = lambda i: jnp.clip(i, 0, n_mlp - 1)
    grp = lambda i: jnp.clip(i - b1, 0, n_grp - 1)
    tqi = lambda i: jnp.clip(i - b2, 0, n_qkv - 1)
    any_spec = pl.BlockSpec(memory_space=pl.ANY)
    in_specs = [
        pl.BlockSpec((n_seq, d), full),
        pl.BlockSpec((1, n_seq, tf), lambda i, ix: (ix[0], 0, mlp(i))),
        pl.BlockSpec((1, n_seq, d), row3),
        pl.BlockSpec((1, n_seq, 384), lambda i, ix: (ix[0], 0, grp(i))),
        pl.BlockSpec((1, n_seq, 384), lambda i, ix: (ix[0], 0, 4 + grp(i))),
        pl.BlockSpec((1, n_seq, 384), lambda i, ix: (ix[0], 0, 8 + grp(i))),
        pl.BlockSpec((1, n_seq, d), row3),
        pl.BlockSpec((tf, d), lambda i, ix: (mlp(i), 0)),
        pl.BlockSpec((d, tf), lambda i, ix: (0, mlp(i - 1))),
        pl.BlockSpec((tp, d), lambda i, ix: (jnp.clip(i - b0, 0, n_proj - 1), 0)),
        pl.BlockSpec((d, tq), lambda i, ix: (0, tqi(i))),
        pl.BlockSpec((1, d), full), pl.BlockSpec((1, d), full),
    ] + [any_spec] * 8
    out_specs = [
        pl.BlockSpec((n_seq, d), full),
        pl.BlockSpec((1, n_seq, tf), lambda i, ix: (ix[0], 0, mlp(i))),
        pl.BlockSpec((1, n_seq, tf), lambda i, ix: (ix[0], 0, mlp(i))),
        pl.BlockSpec((1, n_seq, d), row3),
        pl.BlockSpec((1, n_seq, tq), lambda i, ix: (ix[0], 0, tqi(i))),
        pl.BlockSpec((1, n_seq, d), row3),
        pl.BlockSpec((1, 1, tf), lambda i, ix: (ix[0], 0, mlp(i))),
        pl.BlockSpec((1, 1, tq), lambda i, ix: (ix[0], 0, tqi(i))),
        pl.BlockSpec((1, 8, d), row3),
    ]
    r2 = lambda t: t.reshape(1, -1)
    args = [idx, dy, pre, x1, qkv, qkv, qkv, xs, wdown, wup, wproj.reshape(d, d), wqkv, r2(g1), r2(g2)]
    outs = pl.pallas_call(
        functools.partial(bwd_kernel, n_mlp, n_proj, n_grp, n_qkv),
        grid_spec=pltpu.PrefetchScalarGridSpec(
            num_scalar_prefetch=1, grid=(b2 + n_qkv,), in_specs=in_specs, out_specs=out_specs,
            scratch_shapes=[pltpu.VMEM((n_seq, d), F32), pltpu.VMEM((2, n_seq, tf), BF), pltpu.VMEM((n_seq, d), BF),
                            pltpu.VMEM((n_seq, d), BF), pltpu.VMEM((n_seq, e), BF)]),
        out_shape=[jax.ShapeDtypeStruct((n_seq, d), BF)] + [jax.ShapeDtypeStruct(s.shape, s.dtype) for s in store],
        input_output_aliases={14 + i: 1 + i for i in range(8)},
        compiler_params=pltpu.CompilerParams(dimension_semantics=("arbitrary",), vmem_limit_bytes=60 * 1024 * 1024),
        cost_estimate=pl.CostEstimate(flops=int(36e9), bytes_accessed=int(1.1e8), transcendentals=0),
        name="layer_bwd",
    )(*args, *store)
    return outs[0], tuple(outs[1:])


def fresh(shapes):
    return pl.pallas_call(
        lambda *refs: None,
        out_shape=shapes,
        out_specs=[pl.BlockSpec(memory_space=pl.ANY)] * len(shapes),
        name="fresh",
    )()


def solution(mesh):
    n_stages = mesh.shape['pp']
    last_stage = n_stages - 1
    fwd_pairs = [(source, source + 1) for source in range(n_stages - 1)]
    bwd_pairs = [(source + 1, source) for source in range(n_stages - 1)]
    act_spec = P(None, 'dp', None, None)
    param_specs = tuple(P(*(('pp',) + (None,) * (rank_n - 1))) for rank_n in PARAM_RANKS)
    grad_specs = tuple(P(*((('dp', 'pp'),) + (None,) * (rank_n - 1))) for rank_n in PARAM_RANKS)

    def stage_body(acts_in, cotangent, *stacked_w):
        weights = tuple(tensor[0] for tensor in stacked_w)
        stage = lax.axis_index('pp')
        n_micro, n_rows, n_seq, d = acts_in.shape
        n_chunk = n_micro * n_rows
        x_all = acts_in.reshape(n_chunk, n_seq, d)
        ct_all = cotangent.reshape(n_chunk, n_seq, d)
        sds = jax.ShapeDtypeStruct
        st = lambda r, w, t: sds((n_chunk, r, w), t)
        f = 4 * d
        shapes = [st(n_seq, d, BF), st(n_seq, d, BF), st(n_seq, 3 * d, BF), st(n_seq, d, BF), st(n_seq, d, BF), st(n_seq, d, BF), st(n_seq, f, F32),
                  st(n_seq, f, BF), st(n_seq, f, BF), st(n_seq, d, BF), st(n_seq, 3 * d, BF), st(n_seq, d, BF), st(1, f, F32), st(1, 3 * d, F32), st(8, d, F32),
                  st(n_seq, d, BF), st(n_seq, d, BF)]
        bufs = fresh(shapes)
        saved, store, y_all, dx_all = tuple(bufs[:7]), tuple(bufs[7:15]), bufs[15], bufs[16]
        zero = jnp.zeros((n_seq, d), BF)
        as_idx = lambda c: jnp.reshape(c, (1,)).astype(jnp.int32)

        def forward(t, x_in, saved, y_all):
            c = t - stage
            ok = (c >= 0) & (c < n_chunk)
            c = jnp.clip(c, 0, n_chunk - 1)

            def run(ops):
                x_in, saved, y_all = ops
                first = lax.dynamic_index_in_dim(x_all, c, 0, keepdims=False)
                x = jnp.where(stage == 0, first, x_in)
                y, saved = fwd_call(as_idx(c), x, weights, saved)
                return y, saved, lax.dynamic_update_index_in_dim(y_all, y, c, 0)

            return lax.cond(ok, run, lambda ops: (ops[0], ops[1], ops[2]), (x_in, saved, y_all))

        def backward(t, dy_in, saved, store, dx_all):
            c = t - (2 * last_stage - stage)
            ok = (c >= 0) & (c < n_chunk)
            c = jnp.clip(c, 0, n_chunk - 1)

            def run(ops):
                dy_in, store, dx_all = ops
                top = lax.dynamic_index_in_dim(ct_all, c, 0, keepdims=False)
                dy = jnp.where(stage == last_stage, top, dy_in)
                dx, store = bwd_call(as_idx(c), dy, weights, saved, store)
                return dx, store, lax.dynamic_update_index_in_dim(dx_all, dx, c, 0)

            return lax.cond(ok, run, lambda ops: (ops[0], ops[1], ops[2]), (dy_in, store, dx_all))

        def fill(t, state):
            x_in, saved, y_all = state
            y, saved, y_all = forward(t, x_in, saved, y_all)
            return lax.ppermute(y, 'pp', fwd_pairs), saved, y_all

        def steady(t, state):
            x_in, dx, saved, store, y_all, dx_all = state
            dy_in = lax.ppermute(dx, 'pp', bwd_pairs)
            y, saved, y_all = forward(t, x_in, saved, y_all)
            x_in = lax.ppermute(y, 'pp', fwd_pairs)
            dx, store, dx_all = backward(t, dy_in, saved, store, dx_all)
            return x_in, dx, saved, store, y_all, dx_all

        def drain(t, state):
            dx, store, dx_all = state
            dy_in = lax.ppermute(dx, 'pp', bwd_pairs)
            return backward(t, dy_in, saved, store, dx_all)

        x_in, saved, y_all = lax.fori_loop(0, last_stage, fill, (zero, saved, y_all))
        x_in, dx, saved, store, y_all, dx_all = lax.fori_loop(
            last_stage, last_stage + n_chunk, steady, (x_in, zero, saved, store, y_all, dx_all))
        dx, store, dx_all = lax.fori_loop(
            last_stage + n_chunk, 2 * last_stage + n_chunk, drain, (dx, store, dx_all))

        acts_out = lax.psum(jnp.where(stage == last_stage, y_all, jnp.zeros_like(y_all)), 'pp')
        grad_in = lax.psum(jnp.where(stage == 0, dx_all, jnp.zeros_like(dx_all)), 'pp')
        xs, h1, qkv, mix, x1, h2, pre = saved
        act, dpre, dmid, dqkv, dys, sum_up, sum_qkv, sum_d = store
        wgrad = lambda a, b: jnp.einsum('cka,ckb->ab', a, b, preferred_element_type=F32)
        vec = jnp.sum(sum_d, axis=0)
        grads = (vec[0], vec[1], wgrad(h1, dqkv), jnp.sum(sum_qkv, axis=(0, 1)),
                 wgrad(mix, dmid).reshape(stacked_w[4].shape[1:]), vec[4], vec[2], vec[3],
                 wgrad(h2, dpre), jnp.sum(sum_up, axis=(0, 1)), wgrad(act, dys), vec[5])
        shape4 = acts_in.shape
        return (acts_out.reshape(shape4), grad_in.reshape(shape4)) + tuple(g[None] for g in grads)

    return jax.shard_map(stage_body, mesh=mesh, in_specs=(act_spec, act_spec) + param_specs, out_specs=(act_spec, act_spec) + grad_specs, check_vma=False)
```

```python
import functools
import jax
import jax.numpy as jnp
from jax import lax
from jax.experimental import pallas as pl
from jax.experimental.pallas import tpu as pltpu
from jax.sharding import PartitionSpec as P

LN_EPS = 1e-5
PARAM_RANKS = (2, 2, 3, 2, 4, 2, 2, 2, 3, 2, 3, 2)
BF, F32 = jnp.bfloat16, jnp.float32
LOG2E = 1.4426950408889634
GC0 = 0.7978845608028654
GC1 = GC0 * 0.044715
NT = (((1,), (1,)), ((), ()))
NN = (((1,), (0,)), ((), ()))
TN = (((0,), (0,)), ((), ()))
TQ, TF, TD = 512, 512, 512
ROWS, BLK = 32, 128
NC = 512
HEAD_WIN = ((0, 128), (0, 256), (128, 384), (256, 384))
ANY = pl.BlockSpec(memory_space=pl.ANY)
SCALE = 96.0 ** -0.5
VMEM_LIMIT = 62 * 1024 * 1024


def mm(a, b, dims=NN):
    return lax.dot_general(a, b, dims, preferred_element_type=F32)


def ln_stats(x_wide):
    mean_val = jnp.mean(x_wide, axis=-1, keepdims=True)
    centered = x_wide - mean_val
    variance = jnp.mean(centered * centered, axis=-1, keepdims=True)
    rstd = lax.rsqrt(variance + LN_EPS)
    return centered * rstd, rstd


def ln_back(dh, xhat, rstd, gain):
    dxh = dh * gain
    c1 = jnp.mean(dxh, axis=-1, keepdims=True)
    c2 = jnp.mean(dxh * xhat, axis=-1, keepdims=True)
    return rstd * (dxh - c1 - xhat * c2)


def head_mask(j):
    lo, hi = HEAD_WIN[j]
    lane = lax.broadcasted_iota(jnp.int32, (1, hi - lo), 1) + lo
    keep = (lane >= 96 * j) & (lane < 96 * j + 96)
    return jnp.where(keep, 1.0, 0.0).astype(BF)


def lanes(start, size):
    return pl.ds(pl.multiple_of(start, 128), size)


def join_heads(t):
    return jnp.concatenate([t[0] + t[1][:, :128], t[1][:, 128:] + t[2][:, :128], t[2][:, 128:] + t[3]], axis=1)


def row_blocks(n_seq, body):
    def outer(i, carry):
        for u in range(BLK // ROWS):
            body(pl.ds(pl.multiple_of(i * BLK + u * ROWS, ROWS), ROWS))
        return carry

    lax.fori_loop(0, n_seq // BLK, outer, 0)


def fold8(t):
    return jnp.sum(t.reshape(t.shape[0] // 8, 8, t.shape[1]), axis=0)


def fwd_kernel(idx, x_in, x_all, conv_in, g1, s1, bqkv, bproj, g2, s2, bup, bdown, wqkv, wproj, wup, wdown, *rest):
    n_alias = 11
    (y_o, conv_o, xs_o, h1_o, qkv_o, mix_o, x1_o, h2_o, pre_o, lse_o, act_o,
     x_s, h1_s, qkv_s, mix_s, x1_s, h2_s, act_s, stage_s, pre_s, acc_s, y_s, lse_s, vt_s, ot_s, conv_s, wq_s, wp_s, wu_s, wd_s,
     sem_in, sem_q, sem_u, sem_d, sem_pre, sem_act, sem_out) = rest[n_alias:]
    c, first, last = idx[0], idx[1], idx[2]
    n_seq, d = x_s.shape
    half = n_seq // 2
    n_q, n_f = wqkv.shape[1] // TQ, wup.shape[1] // TF
    copy = pltpu.make_async_copy
    four = lambda j: lax.rem(j, 4)
    wq = lambda j: copy(wqkv.at[:, lanes(j * TQ, TQ)], wq_s.at[lax.rem(j, 6)], sem_q.at[lax.rem(j, 6)])
    act_out = lambda j: copy(stage_s.at[four(j)], act_o.at[c, :, lanes(j * TF, TF)], sem_act.at[four(j)])
    wu = lambda j: copy(wup.at[:, lanes(j * TF, TF)], wu_s.at[four(j)], sem_u.at[four(j)])
    wd = lambda j: copy(wdown.at[pl.ds(pl.multiple_of(j * TF, TF), TF), :], wd_s.at[four(j)], sem_d.at[four(j)])
    pre_out = lambda j: copy(pre_s.at[four(j)], pre_o.at[c, :, lanes(j * TF, TF)], sem_pre.at[four(j)])
    x_copy = copy(x_in, x_s, sem_in.at[0])
    wp_copy = copy(wproj, wp_s, sem_in.at[1])

    @pl.when(first == 1)
    def _():
        copy(x_all.at[c], x_s, sem_in.at[0]).start()

    @pl.when(first == 0)
    def _():
        x_copy.start()

    wq(0).start()
    x_copy.wait()
    for j in range(1, 6):
        wq(j).start()

    def ln_first(rows):
        xhat, _ = ln_stats(x_s[rows].astype(F32))
        h1_s[rows] = (xhat * g1[...].astype(F32) + s1[...].astype(F32)).astype(BF)

    row_blocks(n_seq, ln_first)
    conv_load = copy(conv_in, conv_s, sem_in.at[2])
    conv_put = copy(conv_s, conv_o, sem_in.at[3])

    @pl.when(last == 0)
    def _():
        conv_load.start()

    outs = [copy(x_s, xs_o.at[c], sem_out.at[0]), copy(h1_s, h1_o.at[c], sem_out.at[1])]
    for o in outs:
        o.start()

    def qkv_tiles(i, carry):
        for u in range(3):
            wq(3 * i + u).wait()
        for u in range(3):
            j = 3 * i + u
            cols = lanes(j * TQ, TQ)
            qkv_s[:, cols] = (mm(h1_s[...], wq_s[lax.rem(j, 6)]) + bqkv[:, cols].astype(F32)).astype(BF)
        for u in range(3):
            @pl.when(3 * i + u + 6 < n_q)
            def _(j=3 * i + u + 6):
                wq(j).start()

        return carry

    lax.fori_loop(0, n_q // 3, qkv_tiles, 0)
    wp_copy.start()
    for j in range(4):
        wu(j).start()
        wd(j).start()
    outs.append(copy(qkv_s, qkv_o.at[c], sem_out.at[2]))
    outs[-1].start()

    def attend(grp, carry):
        part = lambda p, lo, hi: qkv_s[:, lanes(p * d + grp * 384 + lo, hi - lo)]
        vt_s[...] = part(2, 0, 384).T
        keep = lax.broadcasted_iota(jnp.int32, (128, 128), 0) <= lax.broadcasted_iota(jnp.int32, (128, 128), 1)
        sc = SCALE * LOG2E

        def scores(j):
            lo, hi = HEAD_WIN[j]
            qm, kw = part(0, lo, hi) * head_mask(j), part(1, lo, hi)
            pre_s[j % 2, :half] = mm(kw[:half], qm, NT)
            pre_s[j % 2, half:, half:] = mm(kw[half:], qm[half:], NT)

        def soften(j):
            for b in range(4):
                cols = slice(b * 128, (b + 1) * 128)

                def block(r):
                    t = pre_s[j % 2, r * 64:(r + 1) * 64, cols] * sc
                    if r // 2 == b:
                        t = jnp.where(keep[(r % 2) * 64:(r % 2 + 1) * 64], t, -1e30)
                    return t.reshape(8, 8, 128)

                n_blk = 2 * (b + 1)
                mx = jnp.max(block(0), axis=0)
                for r in range(1, n_blk):
                    mx = jnp.maximum(mx, jnp.max(block(r), axis=0))
                mx = jnp.max(mx, axis=0, keepdims=True)
                tot = jnp.zeros((8, 128), F32)
                for r in range(n_blk):
                    tot = tot + jnp.sum(jnp.exp2(block(r) - mx), axis=0)
                lse = mx + jnp.log2(jnp.sum(tot, axis=0, keepdims=True))
                lse_s[grp, j:j + 1, cols] = lse
                for r in range(n_blk):
                    act_s[j % 2, r * 64:(r + 1) * 64, cols] = jnp.exp2(block(r) - lse).astype(BF).reshape(64, 128)
                if b % 2 == 0:
                    act_s[j % 2, (b + 1) * 128:(b + 2) * 128, cols] = jnp.zeros((128, 128), BF)

        def mixed(j):
            rows = slice(96 * j, 96 * j + 96)
            ot_s[rows, :half] = mm(vt_s[rows, :half], act_s[j % 2, :half, :half]).astype(BF)
            ot_s[rows, half:] = mm(vt_s[rows, :], act_s[j % 2, :, half:n_seq]).astype(BF)

        scores(0)
        for j in range(4):
            if j < 3:
                scores(j + 1)
            soften(j)
            mixed(j)
        mix_s[:, lanes(grp * 384, 384)] = ot_s[...].T
        return carry

    lax.fori_loop(0, 4, attend, 0)

    @pl.when(last == 0)
    def _():
        conv_load.wait()
        conv_put.start()

    outs.append(copy(mix_s, mix_o.at[c], sem_out.at[3]))
    outs[-1].start()
    outs.append(copy(lse_s, lse_o.at[c], sem_out.at[4]))
    outs[-1].start()
    wp_copy.wait()

    def proj(i, carry):
        cols = lanes(i * NC, NC)
        acc_s[:, cols] = mm(mix_s[...], wp_s[:, cols])
        return carry

    lax.fori_loop(0, d // NC, proj, 0)

    def ln_second(rows):
        x1 = (x_s[rows].astype(F32) + acc_s[rows] + bproj[...].astype(F32)).astype(BF)
        x1_s[rows] = x1
        x1w = x1.astype(F32)
        xhat, _ = ln_stats(x1w)
        h2_s[rows] = (xhat * g2[...].astype(F32) + s2[...].astype(F32)).astype(BF)
        acc_s[rows] = x1w + bdown[...].astype(F32)

    row_blocks(n_seq, ln_second)
    outs.append(copy(x1_s, x1_o.at[c], sem_out.at[5]))
    outs[-1].start()
    outs.append(copy(h2_s, h2_o.at[c], sem_out.at[6]))
    outs[-1].start()

    def up(j, par):
        pre = mm(h2_s[...], wu_s[four(j)]) + bup[:, lanes(j * TF, TF)].astype(F32)
        pre_s[four(j)] = pre
        t = jnp.tanh(pre * (GC0 + GC1 * (pre * pre)))
        a = (0.5 * pre * (1.0 + t)).astype(BF)
        act_s[par] = a
        stage_s[four(j)] = a

    def down(j, par):
        for n in range(0, d, NC):
            acc_s[:, n:n + NC] += mm(act_s[par], wd_s[four(j), :, n:n + NC])

    def put(j):
        pre_out(j).start()
        act_out(j).start()

    def put_done(j):
        pre_out(j).wait()
        act_out(j).wait()

    wu(0).wait()
    up(0, 0)
    put(0)
    wu(4).start()

    def mlp(i, carry):
        j = 1 + 2 * i
        for u in range(2):
            wu(j + u).wait()
            wd(j + u - 1).wait()

            @pl.when(j + u >= 4)
            def _(u=u):
                put_done(j + u - 4)
        for u in range(2):
            up(j + u, (1 + u) % 2)
            down(j + u - 1, u % 2)
        for u in range(2):
            put(j + u)

            @pl.when(j + u + 4 < n_f)
            def _(u=u):
                wu(j + u + 4).start()

            @pl.when(j + u + 3 < n_f)
            def _(u=u):
                wd(j + u + 3).start()
        return carry

    lax.fori_loop(0, (n_f - 2) // 2, mlp, 0)
    j = n_f - 1
    wu(j).wait()
    wd(j - 1).wait()
    wd(j).wait()
    put_done(j - 4)
    up(j, 1)
    down(j - 1, 0)
    put(j)
    for n in range(0, d, NC):
        y_s[:, n:n + NC] = (acc_s[:, n:n + NC] + mm(act_s[1], wd_s[j % 4, :, n:n + NC])).astype(BF)
    y_copy = copy(y_s, y_o, sem_in.at[0])
    y_copy.start()

    @pl.when(last == 1)
    def _():
        copy(y_s, conv_o, sem_in.at[3]).start()

    for o in outs:
        o.wait()
    for i in range(4):
        put_done(j - 3 + i)
    y_copy.wait()

    conv_put.wait()


def fwd_call(idx, x_in, x_all, conv_in, weights, y, conv, saved):
    g1, s1, wqkv, bqkv, wproj, bproj, g2, s2, wup, bup, wdown, bdown = weights
    n_seq, d = x_in.shape
    e, f = wqkv.shape[1], wup.shape[1]
    r2 = lambda t: t.reshape(1, -1)
    vm = pl.BlockSpec(memory_space=pltpu.VMEM)
    args = [idx, x_in, x_all, conv_in, r2(g1), r2(s1), r2(bqkv), r2(bproj), r2(g2), r2(s2), r2(bup), r2(bdown),
            wqkv, wproj.reshape(d, d), wup, wdown]
    alias = [y, conv] + list(saved)
    dma = pltpu.SemaphoreType.DMA
    vmem = lambda *s: pltpu.VMEM(s[:-1], s[-1])
    outs = pl.pallas_call(
        fwd_kernel,
        in_specs=[pl.BlockSpec(memory_space=pltpu.SMEM), ANY, ANY, ANY] + [vm] * 8 + [ANY] * (4 + len(alias)),
        out_specs=[ANY] * len(alias),
        out_shape=[jax.ShapeDtypeStruct(t.shape, t.dtype) for t in alias],
        input_output_aliases={len(args) + i: i for i in range(len(alias))},
        scratch_shapes=[
            vmem(n_seq, d, BF), vmem(n_seq, d, BF), vmem(n_seq, e, BF), vmem(n_seq, d, BF), vmem(n_seq, d, BF), vmem(n_seq, d, BF),
            vmem(2, n_seq, TF, BF), vmem(4, n_seq, TF, BF), vmem(4, n_seq, TF, F32), vmem(n_seq, d, F32), vmem(n_seq, d, BF),
            vmem(4, 8, n_seq, F32), vmem(384, n_seq, BF), vmem(384, n_seq, BF), vmem(n_seq, d, BF),
            vmem(6, d, TQ, BF), vmem(d, d, BF), vmem(4, d, TF, BF), vmem(4, TF, d, BF),
            dma((4,)), dma((6,)), dma((4,)), dma((4,)), dma((4,)), dma((4,)), dma((7,)),
        ],
        compiler_params=pltpu.CompilerParams(vmem_limit_bytes=VMEM_LIMIT),
        cost_estimate=pl.CostEstimate(flops=int(31e9), bytes_accessed=int(9e7), transcendentals=0),
        name="layer_fwd",
    )(*args, *alias)
    return outs[0], outs[1], tuple(outs[2:])


def bwd_kernel(idx, dy_in, ct_all, conv, xs, qkv, mix, x1, pre, lse, g1, g2, wqkv, wproj, wup, wdown, *rest):
    n_alias = 10
    (dx_o, dxs_o, ys_o, dpre_o, dmid_o, dqkv_o, dys_o, sup_o, sqkv_o, sd_o,
     dy_s, acc_s, dp_s, p_s, stage_s, x1_s, dm_s, do_s, qkv_s, mix_s, x_s, conv_s, lse_s, rd_s, kt_s, dqt_s, sup_s, sqkv_s, sd_s, fold_s, pre_s,
     wq_s, wp_s, wu_s, wd_s,
     sem_in, sem_q, sem_u, sem_d, sem_pre, sem_dp, sem_out) = rest[n_alias:]
    c, first, last = idx[0], idx[1], idx[2]
    n_seq, d = dy_s.shape
    half = n_seq // 2
    n_q, n_f = wqkv.shape[1] // TQ, wup.shape[1] // TF
    copy = pltpu.make_async_copy
    four = lambda j: lax.rem(j, 4)
    n_t = wqkv.shape[0] // TD
    wq = lambda j: copy(wqkv.at[pl.ds(pl.multiple_of(j * TD, TD), TD), :], wq_s.at[lax.rem(j, 2)], sem_q.at[lax.rem(j, 2)])
    wu = lambda j: copy(wup.at[:, lanes(j * TF, TF)], wu_s.at[four(j)], sem_u.at[four(j)])
    wd = lambda j: copy(wdown.at[pl.ds(pl.multiple_of(j * TF, TF), TF), :], wd_s.at[four(j)], sem_d.at[four(j)])
    pre_in = lambda j: copy(pre.at[c, :, lanes(j * TF, TF)], pre_s.at[four(j)], sem_pre.at[four(j)])
    dp_out = lambda j: copy(stage_s.at[four(j)], dpre_o.at[c, :, lanes(j * TF, TF)], sem_dp.at[four(j)])
    dy_copy = copy(dy_in, dy_s, sem_in.at[0])
    ins = [copy(x1.at[c], x1_s, sem_in.at[1]), copy(wproj, wp_s, sem_in.at[2]), copy(qkv.at[c], qkv_s, sem_in.at[3]),
           copy(mix.at[c], mix_s, sem_in.at[4]), copy(lse.at[c], lse_s, sem_in.at[5]), copy(xs.at[c], x_s, sem_in.at[6]),
           copy(conv, conv_s, sem_in.at[7])]
    colsum = lambda t: jnp.sum(t, axis=0, keepdims=True)

    @pl.when(last == 1)
    def _():
        copy(ct_all.at[c], dy_s, sem_in.at[0]).start()

    @pl.when(last == 0)
    def _():
        dy_copy.start()

    wd(0).start()
    pre_in(0).start()
    dy_copy.wait()
    for j in range(1, 4):
        wd(j).start()
        pre_in(j).start()
        wu(j - 1).start()
    wu(3).start()
    outs = [copy(dy_s, dys_o.at[c], sem_out.at[0])]
    outs[0].start()

    def down_back(j, par):
        slot = four(j)
        da = mm(dy_s[...], wd_s[slot], NT).astype(BF).astype(F32)
        p = pre_s[slot]
        p2 = p * p
        t = jnp.tanh(p * (GC0 + GC1 * p2))
        dpre = da * ((0.5 + 0.5 * t) * (1.0 + (1.0 - t) * (p * (GC0 + (3.0 * GC1) * p2))))
        sup_s[:, lanes(j * TF, TF)] = colsum(dpre)
        b = dpre.astype(BF)
        dp_s[par] = b
        stage_s[slot] = b

    def up_back(j, par):
        for n in range(0, d, NC):
            acc_s[:, n:n + NC] += mm(dp_s[par], wu_s[four(j), n:n + NC, :], NT)

    wd(0).wait()
    pre_in(0).wait()
    acc_s[...] = jnp.zeros_like(acc_s)
    down_back(0, 0)
    dp_out(0).start()
    wd(4).start()
    pre_in(4).start()

    def mlp(i, carry):
        j = 1 + 2 * i
        for u in range(2):
            wd(j + u).wait()
            pre_in(j + u).wait()
            wu(j + u - 1).wait()

            @pl.when(j + u >= 4)
            def _(u=u):
                dp_out(j + u - 4).wait()
        for u in range(2):
            down_back(j + u, (1 + u) % 2)
            up_back(j + u - 1, u % 2)
        for u in range(2):
            dp_out(j + u).start()

            @pl.when(j + u + 4 < n_f)
            def _(u=u):
                wd(j + u + 4).start()
                pre_in(j + u + 4).start()

            @pl.when(j + u + 3 < n_f)
            def _(u=u):
                wu(j + u + 3).start()

        @pl.when(i == (n_f - 2) // 2 - 1)
        def _():
            for t in ins[:2]:
                t.start()

        return carry

    lax.fori_loop(0, (n_f - 2) // 2, mlp, 0)
    j = n_f - 1
    wd(j).wait()
    pre_in(j).wait()
    wu(j - 1).wait()
    wu(j).wait()
    dp_out(j - 4).wait()
    down_back(j, 1)
    up_back(j - 1, 0)
    dp_out(j).start()
    for t in ins[2:]:
        t.start()
    up_back(j, 1)
    ins[6].wait()
    outs.append(copy(conv_s, ys_o.at[c], sem_out.at[1]))
    outs[-1].start()
    ins[0].wait()

    def ln_bwd(src, base, base2, gain, dst, rows_at):
        fold_s[...] = jnp.zeros_like(fold_s)

        def body(rows):
            dh = acc_s[rows].astype(BF).astype(F32)
            xhat, rstd = ln_stats(src[rows].astype(F32))
            out = (base[rows].astype(F32) + ln_back(dh, xhat, rstd, gain[...].astype(F32))).astype(BF)
            dst[rows] = out
            fold_s[0] += fold8(dh * xhat)
            fold_s[1] += fold8(dh)
            if base2:
                fold_s[2] += fold8(out.astype(F32))
                fold_s[3] += fold8(dy_s[rows].astype(F32))

        row_blocks(n_seq, body)
        for i, at in enumerate(rows_at):
            sd_s[at:at + 1, :] = colsum(fold_s[i])

    ln_bwd(x1_s, dy_s, True, g2, dm_s, (2, 3, 4, 5))
    outs.append(copy(dm_s, dmid_o.at[c], sem_out.at[2]))
    outs[-1].start()
    ins[1].wait()

    def proj(i, carry):
        do_s[:, lanes(i * NC, NC)] = mm(dm_s[...], wp_s[pl.ds(pl.multiple_of(i * NC, NC), NC), :], NT).astype(BF)
        return carry

    lax.fori_loop(0, d // NC, proj, 0)
    for j in range(2):
        wq(j).start()
    for i in range(4):
        dp_out(n_f - 4 + i).wait()
    for t in ins[2:6]:
        t.wait()

    def attend(grp, carry):
        part = lambda p, lo, hi: qkv_s[:, lanes(p * d + grp * 384 + lo, hi - lo)]
        do_at = lambda lo, hi: do_s[:, lanes(grp * 384 + lo, hi - lo)]
        kt_s[...] = part(1, 0, 384).T
        prod = do_at(0, 384).T.astype(F32) * mix_s[:, lanes(grp * 384, 384)].T.astype(F32)
        for j in range(4):
            rd_s[j:j + 1, :] = colsum(prod[96 * j:96 * j + 96])
        causal = lax.broadcasted_iota(jnp.int32, (half, half), 0) <= lax.broadcasted_iota(jnp.int32, (half, half), 1)
        sc = SCALE * LOG2E
        dks, dvs = [], []
        lrow = lse_s[grp]
        def scores(j):
            lo, hi = HEAD_WIN[j]
            m = head_mask(j)
            qm, dom = part(0, lo, hi) * m, do_at(lo, hi) * m
            kw, vw = part(1, lo, hi), part(2, lo, hi)
            for at, a, b in ((0, kw, qm), (2, vw, dom)):
                pre_s[at + j % 2, :half] = mm(a[:half], b, NT)
                pre_s[at + j % 2, half:, half:] = mm(a[half:], b[half:], NT)

        def soften(j):
            for kb, qb in ((0, 0), (0, 1), (1, 1)):
                for r in range(kb * half, (kb + 1) * half, 32):
                    rows, cols = slice(r, r + 32), slice(qb * half, (qb + 1) * half)
                    p = jnp.exp2(pre_s[j % 2, rows, cols] * sc - lrow[j:j + 1, cols])
                    if kb == qb:
                        p = jnp.where(causal[r - kb * half:r - kb * half + 32], p, 0.0)
                    dp = pre_s[2 + j % 2, rows, cols].astype(BF).astype(F32)
                    p_s[j % 2, rows, cols] = p.astype(BF)
                    dp_s[j % 2, rows, cols] = (p * (dp - rd_s[j:j + 1, cols])).astype(BF)

        def products(j):
            lo, hi = HEAD_WIN[j]
            m = head_mask(j)
            qm, dom = part(0, lo, hi) * m, do_at(lo, hi) * m
            rows = slice(96 * j, 96 * j + 96)
            p, ds = p_s.at[j % 2], dp_s.at[j % 2]
            dvs.append(jnp.concatenate([mm(p[:half, :n_seq], dom), mm(p[half:, half:n_seq], dom[half:])], axis=0))
            dks.append(jnp.concatenate([mm(ds[:half, :n_seq], qm), mm(ds[half:, half:n_seq], qm[half:])], axis=0))
            dqt_s[rows, :half] = (mm(kt_s[rows, :half], ds[:half, :half]) * SCALE).astype(BF)
            dqt_s[rows, half:] = (mm(kt_s[rows, :], ds[:, half:n_seq]) * SCALE).astype(BF)

        scores(0)
        for j in range(4):
            if j < 3:
                scores(j + 1)
            soften(j)
            products(j)
        qkv_s[:, lanes(grp * 384, 384)] = dqt_s[...].T
        qkv_s[:, lanes(d + grp * 384, 384)] = (join_heads(dks) * SCALE).astype(BF)
        qkv_s[:, lanes(2 * d + grp * 384, 384)] = join_heads(dvs).astype(BF)
        return carry

    lax.fori_loop(0, 4, attend, 0)
    outs.append(copy(qkv_s, dqkv_o.at[c], sem_out.at[3]))
    outs[-1].start()

    def qkv_back(j, carry):
        wq(j).wait()
        acc_s[:, lanes(j * TD, TD)] = mm(qkv_s[...], wq_s[lax.rem(j, 2)], NT)
        for u in range(3):
            cols = lanes((3 * j + u) * TQ, TQ)
            sqkv_s[:, cols] = colsum(qkv_s[:, cols].astype(F32))

        @pl.when(j + 2 < n_t)
        def _():
            wq(j + 2).start()

        return carry

    lax.fori_loop(0, n_t, qkv_back, 0)
    ln_bwd(x_s, dm_s, False, g1, x1_s, (0, 1))
    dx_copy = copy(x1_s, dx_o, sem_in.at[0])
    dx_copy.start()

    @pl.when(first == 1)
    def _():
        copy(x1_s, dxs_o.at[c], sem_in.at[1]).start()

    sd_s[6:8, :] = jnp.zeros((2, d), F32)
    for i, (src, dst) in enumerate(((sup_s, sup_o), (sqkv_s, sqkv_o), (sd_s, sd_o))):
        outs.append(copy(src, dst.at[c], sem_out.at[4 + i]))
        outs[-1].start()
    for o in outs:
        o.wait()
    dx_copy.wait()

    @pl.when(first == 1)
    def _():
        copy(x1_s, dxs_o.at[c], sem_in.at[1]).wait()


def bwd_call(idx, dy_in, ct_all, conv, weights, saved, dx, dx_all, y_all, store):
    g1, s1, wqkv, bqkv, wproj, bproj, g2, s2, wup, bup, wdown, bdown = weights
    xs, h1, qkv, mix, x1, h2, pre, lse, act = saved
    n_seq, d = dy_in.shape
    e, f = wqkv.shape[1], wup.shape[1]
    r2 = lambda t: t.reshape(1, -1)
    vm = pl.BlockSpec(memory_space=pltpu.VMEM)
    args = [idx, dy_in, ct_all, conv, xs, qkv, mix, x1, pre, lse, r2(g1), r2(g2), wqkv, wproj.reshape(d, d), wup, wdown]
    alias = [dx, dx_all, y_all] + list(store)
    dma = pltpu.SemaphoreType.DMA
    vmem = lambda *s: pltpu.VMEM(s[:-1], s[-1])
    outs = pl.pallas_call(
        bwd_kernel,
        in_specs=[pl.BlockSpec(memory_space=pltpu.SMEM)] + [ANY] * 9 + [vm] * 2 + [ANY] * (4 + len(alias)),
        out_specs=[ANY] * len(alias),
        out_shape=[jax.ShapeDtypeStruct(t.shape, t.dtype) for t in alias],
        input_output_aliases={len(args) + i: i for i in range(len(alias))},
        scratch_shapes=[
            vmem(n_seq, d, BF), vmem(n_seq, d, F32), vmem(2, n_seq, TF, BF), vmem(2, n_seq, n_seq, BF), vmem(4, n_seq, TF, BF), vmem(n_seq, d, BF), vmem(n_seq, d, BF),
            vmem(n_seq, d, BF), vmem(n_seq, e, BF), vmem(n_seq, d, BF), vmem(n_seq, d, BF),
            vmem(n_seq, d, BF), vmem(4, 8, n_seq, F32), vmem(8, n_seq, F32), vmem(384, n_seq, BF), vmem(384, n_seq, BF), vmem(1, f, F32), vmem(1, e, F32), vmem(8, d, F32), vmem(4, 8, d, F32),
            vmem(4, n_seq, TF, F32), vmem(2, TD, e, BF), vmem(d, d, BF), vmem(4, d, TF, BF), vmem(4, TF, d, BF),
            dma((8,)), dma((2,)), dma((4,)), dma((4,)), dma((4,)), dma((4,)), dma((7,)),
        ],
        compiler_params=pltpu.CompilerParams(vmem_limit_bytes=VMEM_LIMIT),
        cost_estimate=pl.CostEstimate(flops=int(36e9), bytes_accessed=int(1.1e8), transcendentals=0),
        name="layer_bwd",
    )(*args, *alias)
    return outs[0], outs[1], outs[2], tuple(outs[3:])


def fresh(shapes):
    return pl.pallas_call(
        lambda *refs: None,
        out_shape=shapes,
        out_specs=[ANY] * len(shapes),
        name="fresh",
    )()


def relay_kernel(src, _alias, dst, buf, sems):
    load = pltpu.make_async_copy(src, buf, sems.at[0])
    load.start()
    load.wait()
    put = pltpu.make_async_copy(buf, dst, sems.at[1])
    put.start()
    put.wait()


def relay(src, dst):
    return pl.pallas_call(
        relay_kernel,
        in_specs=[ANY, ANY],
        out_specs=ANY,
        out_shape=jax.ShapeDtypeStruct(dst.shape, dst.dtype),
        input_output_aliases={1: 0},
        scratch_shapes=[pltpu.VMEM(src.shape, src.dtype), pltpu.SemaphoreType.DMA((2,))],
        name="relay",
    )(src, dst)


def solution(mesh):
    n_stages = mesh.shape['pp']
    last_stage = n_stages - 1
    fwd_pairs = [(source, source + 1) for source in range(n_stages - 1)]
    bwd_pairs = [(source + 1, source) for source in range(n_stages - 1)]
    act_spec = P(None, 'dp', None, None)
    param_specs = tuple(P(*(('pp',) + (None,) * (rank_n - 1))) for rank_n in PARAM_RANKS)
    grad_specs = tuple(P(*((('dp', 'pp'),) + (None,) * (rank_n - 1))) for rank_n in PARAM_RANKS)

    def stage_body(acts_in, cotangent, *stacked_w):
        weights = tuple(tensor[0] for tensor in stacked_w)
        stage = lax.axis_index('pp')
        n_micro, n_rows, n_seq, d = acts_in.shape
        n_chunk = n_micro * n_rows
        x_all = acts_in.reshape(n_chunk, n_seq, d)
        ct_all = cotangent.reshape(n_chunk, n_seq, d)
        f = 4 * d
        sds = jax.ShapeDtypeStruct
        many = lambda w, t=BF: sds((n_chunk, n_seq, w), t)
        tall = lambda r, w: sds((n_chunk, r, w), F32)
        one = sds((n_seq, d), BF)
        shapes = [many(d), many(d), many(3 * d), many(d), many(d), many(d), many(f, F32), sds((n_chunk, 4, 8, n_seq), F32), many(f),
                  many(f), many(d), many(3 * d), many(d), tall(1, f), tall(1, 3 * d), tall(8, d),
                  many(d), many(d), one, one, one, one, one]
        bufs = fresh(shapes)
        saved, store = tuple(bufs[:9]), tuple(bufs[9:16])
        dx_all, y_all, x_in, conv_in, y, dx, conv = bufs[16:]

        def forward(t, x_in, conv_in, y, conv, saved):
            c = t - stage
            ok = (c >= 0) & (c < n_chunk)
            idx = jnp.stack([jnp.clip(c, 0, n_chunk - 1), stage == 0, stage == last_stage]).astype(jnp.int32)
            run = lambda x_in, conv_in, y, conv, saved: fwd_call(idx, x_in, x_all, conv_in, weights, y, conv, saved)
            skip = lambda x_in, conv_in, y, conv, saved: (y, relay(conv_in, conv), saved)
            return lax.cond(ok, run, skip, x_in, conv_in, y, conv, saved)

        def backward(t, dy_in, conv, saved, dx, dx_all, y_all, store):
            c = t - (2 * last_stage - stage)
            ok = (c >= 0) & (c < n_chunk)
            idx = jnp.stack([jnp.clip(c, 0, n_chunk - 1), stage == 0, stage == last_stage]).astype(jnp.int32)
            run = lambda dy_in, conv, saved, dx, dx_all, y_all, store: bwd_call(idx, dy_in, ct_all, conv, weights, saved, dx, dx_all, y_all, store)
            skip = lambda dy_in, conv, saved, dx, dx_all, y_all, store: (dx, dx_all, y_all, store)
            return lax.cond(ok, run, skip, dy_in, conv, saved, dx, dx_all, y_all, store)

        def step(t, state):
            x_in, conv_in, y, dx, conv, saved, store, dx_all, y_all = state
            dy_in = lax.ppermute(dx, 'pp', bwd_pairs)
            y, conv, saved = forward(t, x_in, conv_in, y, conv, saved)
            x_in = lax.ppermute(y, 'pp', fwd_pairs)
            conv_in = lax.ppermute(conv, 'pp', bwd_pairs)
            dx, dx_all, y_all, store = backward(t, dy_in, conv, saved, dx, dx_all, y_all, store)
            return x_in, conv_in, y, dx, conv, saved, store, dx_all, y_all

        state = (x_in, conv_in, y, dx, conv, saved, store, dx_all, y_all)
        x_in, conv_in, y, dx, conv, saved, store, dx_all, y_all = lax.fori_loop(0, n_chunk + 2 * last_stage, step, state)

        grad_in = lax.psum(jnp.where(stage == 0, dx_all, jnp.zeros_like(dx_all)), 'pp')
        xs, h1, qkv, mix, x1, h2, pre, lse, act = saved
        dpre, dmid, dqkv, dys, sum_up, sum_qkv, sum_d = store
        wgrad = lambda a, b: jnp.einsum('cka,ckb->ab', a, b, preferred_element_type=F32)
        vec = jnp.sum(sum_d, axis=0)
        grads = (vec[0], vec[1], wgrad(h1, dqkv), jnp.sum(sum_qkv, axis=(0, 1)),
                 wgrad(mix, dmid).reshape(stacked_w[4].shape[1:]), vec[4], vec[2], vec[3],
                 wgrad(h2, dpre), jnp.sum(sum_up, axis=(0, 1)), wgrad(act, dys), vec[5])
        shape4 = acts_in.shape
        return (y_all.reshape(shape4), grad_in.reshape(shape4)) + tuple(g[None] for g in grads)

    return jax.shard_map(stage_body, mesh=mesh, in_specs=(act_spec, act_spec) + param_specs, out_specs=(act_spec, act_spec) + grad_specs, check_vma=False)
```

```python
import functools
import jax
import jax.numpy as jnp
from jax import lax
from jax.experimental import pallas as pl
from jax.experimental.pallas import tpu as pltpu
from jax.sharding import PartitionSpec as P

LN_EPS = 1e-5
PARAM_RANKS = (2, 2, 3, 2, 4, 2, 2, 2, 3, 2, 3, 2)
BF, F32 = jnp.bfloat16, jnp.float32
LOG2E = 1.4426950408889634
GC0 = 0.7978845608028654
GC1 = GC0 * 0.044715
NT = (((1,), (1,)), ((), ()))
NN = (((1,), (0,)), ((), ()))
TN = (((0,), (0,)), ((), ()))
TQ, TF, TD = 512, 512, 512
ROWS, BLK = 32, 128
NC = 512
HEAD_WIN = ((0, 128), (0, 256), (128, 384), (256, 384))
ANY = pl.BlockSpec(memory_space=pl.ANY)
SCALE = 96.0 ** -0.5
VMEM_LIMIT = 62 * 1024 * 1024


def mm(a, b, dims=NN):
    return lax.dot_general(a, b, dims, preferred_element_type=F32)


def ln_stats(x_wide):
    mean_val = jnp.mean(x_wide, axis=-1, keepdims=True)
    centered = x_wide - mean_val
    variance = jnp.mean(centered * centered, axis=-1, keepdims=True)
    rstd = lax.rsqrt(variance + LN_EPS)
    return centered * rstd, rstd


def ln_back(dh, xhat, rstd, gain):
    dxh = dh * gain
    c1 = jnp.mean(dxh, axis=-1, keepdims=True)
    c2 = jnp.mean(dxh * xhat, axis=-1, keepdims=True)
    return rstd * (dxh - c1 - xhat * c2)


def head_mask(j):
    lo, hi = HEAD_WIN[j]
    lane = lax.broadcasted_iota(jnp.int32, (1, hi - lo), 1) + lo
    keep = (lane >= 96 * j) & (lane < 96 * j + 96)
    return jnp.where(keep, 1.0, 0.0).astype(BF)


def lanes(start, size):
    return pl.ds(pl.multiple_of(start, 128), size)


def join_heads(t):
    return jnp.concatenate([t[0] + t[1][:, :128], t[1][:, 128:] + t[2][:, :128], t[2][:, 128:] + t[3]], axis=1)


def row_blocks(n_seq, body):
    def outer(i, carry):
        for u in range(BLK // ROWS):
            body(pl.ds(pl.multiple_of(i * BLK + u * ROWS, ROWS), ROWS))
        return carry

    lax.fori_loop(0, n_seq // BLK, outer, 0)


def fold8(t):
    return jnp.sum(t.reshape(t.shape[0] // 8, 8, t.shape[1]), axis=0)


def fwd_kernel(idx, x_in, x_all, g1, s1, bqkv, bproj, g2, s2, bup, bdown, wqkv, wproj, wup, wdown, *rest):
    n_alias = 11
    (y_o, ys_o, xs_o, h1_o, qkv_o, mix_o, x1_o, h2_o, pre_o, lse_o, act_o,
     x_s, h1_s, qkv_s, mix_s, x1_s, h2_s, act_s, stage_s, pre_s, acc_s, y_s, lse_s, vt_s, ot_s, zero_s, wq_s, wp_s, wu_s, wd_s,
     sem_in, sem_q, sem_u, sem_d, sem_pre, sem_act, sem_out) = rest[n_alias:]
    c, first, last = idx[0], idx[1], idx[2]
    n_seq, d = x_s.shape
    half = n_seq // 2
    n_q, n_f = wqkv.shape[1] // TQ, wup.shape[1] // TF
    copy = pltpu.make_async_copy
    four = lambda j: lax.rem(j, 4)
    wq = lambda j: copy(wqkv.at[:, lanes(j * TQ, TQ)], wq_s.at[lax.rem(j, 6)], sem_q.at[lax.rem(j, 6)])
    act_out = lambda j: copy(stage_s.at[four(j)], act_o.at[c, :, lanes(j * TF, TF)], sem_act.at[four(j)])
    wu = lambda j: copy(wup.at[:, lanes(j * TF, TF)], wu_s.at[four(j)], sem_u.at[four(j)])
    wd = lambda j: copy(wdown.at[pl.ds(pl.multiple_of(j * TF, TF), TF), :], wd_s.at[four(j)], sem_d.at[four(j)])
    pre_out = lambda j: copy(pre_s.at[four(j)], pre_o.at[c, :, lanes(j * TF, TF)], sem_pre.at[four(j)])
    x_copy = copy(x_in, x_s, sem_in.at[0])
    wp_copy = copy(wproj, wp_s, sem_in.at[2])

    @pl.when(first == 1)
    def _():
        copy(x_all.at[c], x_s, sem_in.at[0]).start()

    @pl.when(first == 0)
    def _():
        x_copy.start()

    wq(0).start()
    x_copy.wait()
    for j in range(1, 6):
        wq(j).start()

    def ln_first(rows):
        xhat, _ = ln_stats(x_s[rows].astype(F32))
        h1_s[rows] = (xhat * g1[...].astype(F32) + s1[...].astype(F32)).astype(BF)

    row_blocks(n_seq, ln_first)
    zero_put = copy(zero_s, ys_o.at[c], sem_in.at[1])

    @pl.when(last == 0)
    def _():
        zero_s[...] = jnp.zeros_like(zero_s)
        zero_put.start()

    outs = [copy(x_s, xs_o.at[c], sem_out.at[0]), copy(h1_s, h1_o.at[c], sem_out.at[1])]
    for o in outs:
        o.start()

    def qkv_tiles(i, carry):
        for u in range(3):
            wq(3 * i + u).wait()
        for u in range(3):
            j = 3 * i + u
            cols = lanes(j * TQ, TQ)
            qkv_s[:, cols] = (mm(h1_s[...], wq_s[lax.rem(j, 6)]) + bqkv[:, cols].astype(F32)).astype(BF)
        for u in range(3):
            @pl.when(3 * i + u + 6 < n_q)
            def _(j=3 * i + u + 6):
                wq(j).start()

        return carry

    lax.fori_loop(0, n_q // 3, qkv_tiles, 0)
    wp_copy.start()
    for j in range(4):
        wu(j).start()
        wd(j).start()
    outs.append(copy(qkv_s, qkv_o.at[c], sem_out.at[2]))
    outs[-1].start()

    def attend(grp, carry):
        part = lambda p, lo, hi: qkv_s[:, lanes(p * d + grp * 384 + lo, hi - lo)]
        vt_s[...] = part(2, 0, 384).T
        keep = lax.broadcasted_iota(jnp.int32, (128, 128), 0) <= lax.broadcasted_iota(jnp.int32, (128, 128), 1)
        sc = SCALE * LOG2E

        def scores(j):
            lo, hi = HEAD_WIN[j]
            qm, kw = part(0, lo, hi) * head_mask(j), part(1, lo, hi)
            pre_s[j % 2, :half] = mm(kw[:half], qm, NT)
            pre_s[j % 2, half:, half:] = mm(kw[half:], qm[half:], NT)

        def soften(j):
            for b in range(4):
                cols = slice(b * 128, (b + 1) * 128)

                def block(r):
                    t = pre_s[j % 2, r * 64:(r + 1) * 64, cols] * sc
                    if r // 2 == b:
                        t = jnp.where(keep[(r % 2) * 64:(r % 2 + 1) * 64], t, -1e30)
                    return t.reshape(8, 8, 128)

                n_blk = 2 * (b + 1)
                mx = jnp.max(block(0), axis=0)
                for r in range(1, n_blk):
                    mx = jnp.maximum(mx, jnp.max(block(r), axis=0))
                mx = jnp.max(mx, axis=0, keepdims=True)
                tot = jnp.zeros((8, 128), F32)
                for r in range(n_blk):
                    tot = tot + jnp.sum(jnp.exp2(block(r) - mx), axis=0)
                lse = mx + jnp.log2(jnp.sum(tot, axis=0, keepdims=True))
                lse_s[grp, j:j + 1, cols] = lse
                for r in range(n_blk):
                    act_s[j % 2, r * 64:(r + 1) * 64, cols] = jnp.exp2(block(r) - lse).astype(BF).reshape(64, 128)
                if b % 2 == 0:
                    act_s[j % 2, (b + 1) * 128:(b + 2) * 128, cols] = jnp.zeros((128, 128), BF)

        def mixed(j):
            rows = slice(96 * j, 96 * j + 96)
            ot_s[rows, :half] = mm(vt_s[rows, :half], act_s[j % 2, :half, :half]).astype(BF)
            ot_s[rows, half:] = mm(vt_s[rows, :], act_s[j % 2, :, half:n_seq]).astype(BF)

        scores(0)
        for j in range(4):
            if j < 3:
                scores(j + 1)
            soften(j)
            mixed(j)
        mix_s[:, lanes(grp * 384, 384)] = ot_s[...].T
        return carry

    lax.fori_loop(0, 4, attend, 0)
    outs.append(copy(mix_s, mix_o.at[c], sem_out.at[3]))
    outs[-1].start()
    outs.append(copy(lse_s, lse_o.at[c], sem_out.at[4]))
    outs[-1].start()
    wp_copy.wait()

    def proj(i, carry):
        cols = lanes(i * NC, NC)
        acc_s[:, cols] = mm(mix_s[...], wp_s[:, cols])
        return carry

    lax.fori_loop(0, d // NC, proj, 0)

    def ln_second(rows):
        x1 = (x_s[rows].astype(F32) + acc_s[rows] + bproj[...].astype(F32)).astype(BF)
        x1_s[rows] = x1
        x1w = x1.astype(F32)
        xhat, _ = ln_stats(x1w)
        h2_s[rows] = (xhat * g2[...].astype(F32) + s2[...].astype(F32)).astype(BF)
        acc_s[rows] = x1w + bdown[...].astype(F32)

    row_blocks(n_seq, ln_second)
    outs.append(copy(x1_s, x1_o.at[c], sem_out.at[5]))
    outs[-1].start()
    outs.append(copy(h2_s, h2_o.at[c], sem_out.at[6]))
    outs[-1].start()

    def up(j, par):
        pre = mm(h2_s[...], wu_s[four(j)]) + bup[:, lanes(j * TF, TF)].astype(F32)
        pre_s[four(j)] = pre
        t = jnp.tanh(pre * (GC0 + GC1 * (pre * pre)))
        a = (0.5 * pre * (1.0 + t)).astype(BF)
        act_s[par] = a
        stage_s[four(j)] = a

    def down(j, par):
        for n in range(0, d, NC):
            acc_s[:, n:n + NC] += mm(act_s[par], wd_s[four(j), :, n:n + NC])

    def put(j):
        pre_out(j).start()
        act_out(j).start()

    def put_done(j):
        pre_out(j).wait()
        act_out(j).wait()

    wu(0).wait()
    up(0, 0)
    put(0)
    wu(4).start()

    def mlp(i, carry):
        j = 1 + 2 * i
        for u in range(2):
            wu(j + u).wait()
            wd(j + u - 1).wait()

            @pl.when(j + u >= 4)
            def _(u=u):
                put_done(j + u - 4)
        for u in range(2):
            up(j + u, (1 + u) % 2)
            down(j + u - 1, u % 2)
        for u in range(2):
            put(j + u)

            @pl.when(j + u + 4 < n_f)
            def _(u=u):
                wu(j + u + 4).start()

            @pl.when(j + u + 3 < n_f)
            def _(u=u):
                wd(j + u + 3).start()
        return carry

    lax.fori_loop(0, (n_f - 2) // 2, mlp, 0)
    j = n_f - 1
    wu(j).wait()
    wd(j - 1).wait()
    wd(j).wait()
    put_done(j - 4)
    up(j, 1)
    down(j - 1, 0)
    put(j)
    for n in range(0, d, NC):
        y_s[:, n:n + NC] = (acc_s[:, n:n + NC] + mm(act_s[1], wd_s[j % 4, :, n:n + NC])).astype(BF)
    y_copy = copy(y_s, y_o, sem_in.at[0])
    y_copy.start()

    @pl.when(last == 1)
    def _():
        copy(y_s, ys_o.at[c], sem_in.at[1]).start()

    for o in outs:
        o.wait()
    for i in range(4):
        put_done(j - 3 + i)
    y_copy.wait()

    zero_put.wait()


def fwd_call(idx, x_in, x_all, weights, y, y_all, saved):
    g1, s1, wqkv, bqkv, wproj, bproj, g2, s2, wup, bup, wdown, bdown = weights
    n_seq, d = x_in.shape
    e, f = wqkv.shape[1], wup.shape[1]
    r2 = lambda t: t.reshape(1, -1)
    vm = pl.BlockSpec(memory_space=pltpu.VMEM)
    args = [idx, x_in, x_all, r2(g1), r2(s1), r2(bqkv), r2(bproj), r2(g2), r2(s2), r2(bup), r2(bdown),
            wqkv, wproj.reshape(d, d), wup, wdown]
    alias = [y, y_all] + list(saved)
    dma = pltpu.SemaphoreType.DMA
    vmem = lambda *s: pltpu.VMEM(s[:-1], s[-1])
    outs = pl.pallas_call(
        fwd_kernel,
        in_specs=[pl.BlockSpec(memory_space=pltpu.SMEM), ANY, ANY] + [vm] * 8 + [ANY] * (4 + len(alias)),
        out_specs=[ANY] * len(alias),
        out_shape=[jax.ShapeDtypeStruct(t.shape, t.dtype) for t in alias],
        input_output_aliases={len(args) + i: i for i in range(len(alias))},
        scratch_shapes=[
            vmem(n_seq, d, BF), vmem(n_seq, d, BF), vmem(n_seq, e, BF), vmem(n_seq, d, BF), vmem(n_seq, d, BF), vmem(n_seq, d, BF),
            vmem(2, n_seq, TF, BF), vmem(4, n_seq, TF, BF), vmem(4, n_seq, TF, F32), vmem(n_seq, d, F32), vmem(n_seq, d, BF),
            vmem(4, 8, n_seq, F32), vmem(384, n_seq, BF), vmem(384, n_seq, BF), vmem(n_seq, d, BF),
            vmem(6, d, TQ, BF), vmem(d, d, BF), vmem(4, d, TF, BF), vmem(4, TF, d, BF),
            dma((3,)), dma((6,)), dma((4,)), dma((4,)), dma((4,)), dma((4,)), dma((7,)),
        ],
        compiler_params=pltpu.CompilerParams(vmem_limit_bytes=VMEM_LIMIT),
        cost_estimate=pl.CostEstimate(flops=int(31e9), bytes_accessed=int(9e7), transcendentals=0),
        name="layer_fwd",
    )(*args, *alias)
    return outs[0], outs[1], tuple(outs[2:])


def bwd_kernel(idx, dy_in, ct_all, xs, qkv, mix, x1, pre, lse, g1, g2, wqkv, wproj, wup, wdown, *rest):
    n_alias = 9
    (dx_o, dxs_o, dpre_o, dmid_o, dqkv_o, dys_o, sup_o, sqkv_o, sd_o,
     dy_s, acc_s, dp_s, p_s, stage_s, x1_s, dm_s, do_s, qkv_s, mix_s, x_s, zero_s, lse_s, rd_s, kt_s, dqt_s, sup_s, sqkv_s, sd_s, fold_s, pre_s,
     wq_s, wp_s, wu_s, wd_s,
     sem_in, sem_q, sem_u, sem_d, sem_pre, sem_dp, sem_out) = rest[n_alias:]
    c, first, last = idx[0], idx[1], idx[2]
    n_seq, d = dy_s.shape
    half = n_seq // 2
    n_q, n_f = wqkv.shape[1] // TQ, wup.shape[1] // TF
    copy = pltpu.make_async_copy
    four = lambda j: lax.rem(j, 4)
    n_t = wqkv.shape[0] // TD
    wq = lambda j: copy(wqkv.at[pl.ds(pl.multiple_of(j * TD, TD), TD), :], wq_s.at[lax.rem(j, 2)], sem_q.at[lax.rem(j, 2)])
    wu = lambda j: copy(wup.at[:, lanes(j * TF, TF)], wu_s.at[four(j)], sem_u.at[four(j)])
    wd = lambda j: copy(wdown.at[pl.ds(pl.multiple_of(j * TF, TF), TF), :], wd_s.at[four(j)], sem_d.at[four(j)])
    pre_in = lambda j: copy(pre.at[c, :, lanes(j * TF, TF)], pre_s.at[four(j)], sem_pre.at[four(j)])
    dp_out = lambda j: copy(stage_s.at[four(j)], dpre_o.at[c, :, lanes(j * TF, TF)], sem_dp.at[four(j)])
    dy_copy = copy(dy_in, dy_s, sem_in.at[0])
    ins = [copy(x1.at[c], x1_s, sem_in.at[1]), copy(wproj, wp_s, sem_in.at[2]), copy(qkv.at[c], qkv_s, sem_in.at[3]),
           copy(mix.at[c], mix_s, sem_in.at[4]), copy(lse.at[c], lse_s, sem_in.at[5]), copy(xs.at[c], x_s, sem_in.at[6])]
    zero_put = copy(zero_s, dxs_o.at[c], sem_in.at[7])
    colsum = lambda t: jnp.sum(t, axis=0, keepdims=True)

    @pl.when(last == 1)
    def _():
        copy(ct_all.at[c], dy_s, sem_in.at[0]).start()

    @pl.when(last == 0)
    def _():
        dy_copy.start()

    wd(0).start()
    pre_in(0).start()
    dy_copy.wait()
    for j in range(1, 4):
        wd(j).start()
        pre_in(j).start()
        wu(j - 1).start()
    wu(3).start()
    outs = [copy(dy_s, dys_o.at[c], sem_out.at[0])]
    outs[0].start()

    def down_back(j, par):
        slot = four(j)
        da = mm(dy_s[...], wd_s[slot], NT).astype(BF).astype(F32)
        p = pre_s[slot]
        p2 = p * p
        t = jnp.tanh(p * (GC0 + GC1 * p2))
        dpre = da * ((0.5 + 0.5 * t) * (1.0 + (1.0 - t) * (p * (GC0 + (3.0 * GC1) * p2))))
        sup_s[:, lanes(j * TF, TF)] = colsum(dpre)
        b = dpre.astype(BF)
        dp_s[par] = b
        stage_s[slot] = b

    def up_back(j, par):
        for n in range(0, d, NC):
            acc_s[:, n:n + NC] += mm(dp_s[par], wu_s[four(j), n:n + NC, :], NT)

    wd(0).wait()
    pre_in(0).wait()
    acc_s[...] = jnp.zeros_like(acc_s)
    down_back(0, 0)
    dp_out(0).start()
    wd(4).start()
    pre_in(4).start()

    def mlp(i, carry):
        j = 1 + 2 * i
        for u in range(2):
            wd(j + u).wait()
            pre_in(j + u).wait()
            wu(j + u - 1).wait()

            @pl.when(j + u >= 4)
            def _(u=u):
                dp_out(j + u - 4).wait()
        for u in range(2):
            down_back(j + u, (1 + u) % 2)
            up_back(j + u - 1, u % 2)
        for u in range(2):
            dp_out(j + u).start()

            @pl.when(j + u + 4 < n_f)
            def _(u=u):
                wd(j + u + 4).start()
                pre_in(j + u + 4).start()

            @pl.when(j + u + 3 < n_f)
            def _(u=u):
                wu(j + u + 3).start()

        @pl.when(i == (n_f - 2) // 2 - 1)
        def _():
            for t in ins[:2]:
                t.start()

        return carry

    lax.fori_loop(0, (n_f - 2) // 2, mlp, 0)
    j = n_f - 1
    wd(j).wait()
    pre_in(j).wait()
    wu(j - 1).wait()
    wu(j).wait()
    dp_out(j - 4).wait()
    down_back(j, 1)
    up_back(j - 1, 0)
    dp_out(j).start()
    for t in ins[2:]:
        t.start()
    up_back(j, 1)

    @pl.when(first == 0)
    def _():
        zero_s[...] = jnp.zeros_like(zero_s)
        zero_put.start()

    ins[0].wait()

    def ln_bwd(src, base, base2, gain, dst, rows_at):
        fold_s[...] = jnp.zeros_like(fold_s)

        def body(rows):
            dh = acc_s[rows].astype(BF).astype(F32)
            xhat, rstd = ln_stats(src[rows].astype(F32))
            out = (base[rows].astype(F32) + ln_back(dh, xhat, rstd, gain[...].astype(F32))).astype(BF)
            dst[rows] = out
            fold_s[0] += fold8(dh * xhat)
            fold_s[1] += fold8(dh)
            if base2:
                fold_s[2] += fold8(out.astype(F32))
                fold_s[3] += fold8(dy_s[rows].astype(F32))

        row_blocks(n_seq, body)
        for i, at in enumerate(rows_at):
            sd_s[at:at + 1, :] = colsum(fold_s[i])

    ln_bwd(x1_s, dy_s, True, g2, dm_s, (2, 3, 4, 5))
    outs.append(copy(dm_s, dmid_o.at[c], sem_out.at[2]))
    outs[-1].start()
    ins[1].wait()

    def proj(i, carry):
        do_s[:, lanes(i * NC, NC)] = mm(dm_s[...], wp_s[pl.ds(pl.multiple_of(i * NC, NC), NC), :], NT).astype(BF)
        return carry

    lax.fori_loop(0, d // NC, proj, 0)
    for j in range(2):
        wq(j).start()
    for i in range(4):
        dp_out(n_f - 4 + i).wait()
    for t in ins[2:6]:
        t.wait()

    def attend(grp, carry):
        part = lambda p, lo, hi: qkv_s[:, lanes(p * d + grp * 384 + lo, hi - lo)]
        do_at = lambda lo, hi: do_s[:, lanes(grp * 384 + lo, hi - lo)]
        kt_s[...] = part(1, 0, 384).T
        prod = do_at(0, 384).T.astype(F32) * mix_s[:, lanes(grp * 384, 384)].T.astype(F32)
        for j in range(4):
            rd_s[j:j + 1, :] = colsum(prod[96 * j:96 * j + 96])
        causal = lax.broadcasted_iota(jnp.int32, (half, half), 0) <= lax.broadcasted_iota(jnp.int32, (half, half), 1)
        sc = SCALE * LOG2E
        dks, dvs = [], []
        lrow = lse_s[grp]
        def scores(j):
            lo, hi = HEAD_WIN[j]
            m = head_mask(j)
            qm, dom = part(0, lo, hi) * m, do_at(lo, hi) * m
            kw, vw = part(1, lo, hi), part(2, lo, hi)
            for at, a, b in ((0, kw, qm), (2, vw, dom)):
                pre_s[at + j % 2, :half] = mm(a[:half], b, NT)
                pre_s[at + j % 2, half:, half:] = mm(a[half:], b[half:], NT)

        def soften(j):
            for kb, qb in ((0, 0), (0, 1), (1, 1)):
                for r in range(kb * half, (kb + 1) * half, 32):
                    rows, cols = slice(r, r + 32), slice(qb * half, (qb + 1) * half)
                    p = jnp.exp2(pre_s[j % 2, rows, cols] * sc - lrow[j:j + 1, cols])
                    if kb == qb:
                        p = jnp.where(causal[r - kb * half:r - kb * half + 32], p, 0.0)
                    dp = pre_s[2 + j % 2, rows, cols].astype(BF).astype(F32)
                    p_s[j % 2, rows, cols] = p.astype(BF)
                    dp_s[j % 2, rows, cols] = (p * (dp - rd_s[j:j + 1, cols])).astype(BF)

        def products(j):
            lo, hi = HEAD_WIN[j]
            m = head_mask(j)
            qm, dom = part(0, lo, hi) * m, do_at(lo, hi) * m
            rows = slice(96 * j, 96 * j + 96)
            p, ds = p_s.at[j % 2], dp_s.at[j % 2]
            dvs.append(jnp.concatenate([mm(p[:half, :n_seq], dom), mm(p[half:, half:n_seq], dom[half:])], axis=0))
            dks.append(jnp.concatenate([mm(ds[:half, :n_seq], qm), mm(ds[half:, half:n_seq], qm[half:])], axis=0))
            dqt_s[rows, :half] = (mm(kt_s[rows, :half], ds[:half, :half]) * SCALE).astype(BF)
            dqt_s[rows, half:] = (mm(kt_s[rows, :], ds[:, half:n_seq]) * SCALE).astype(BF)

        scores(0)
        for j in range(4):
            if j < 3:
                scores(j + 1)
            soften(j)
            products(j)
        qkv_s[:, lanes(grp * 384, 384)] = dqt_s[...].T
        qkv_s[:, lanes(d + grp * 384, 384)] = (join_heads(dks) * SCALE).astype(BF)
        qkv_s[:, lanes(2 * d + grp * 384, 384)] = join_heads(dvs).astype(BF)
        return carry

    lax.fori_loop(0, 4, attend, 0)
    outs.append(copy(qkv_s, dqkv_o.at[c], sem_out.at[3]))
    outs[-1].start()

    def qkv_back(j, carry):
        wq(j).wait()
        acc_s[:, lanes(j * TD, TD)] = mm(qkv_s[...], wq_s[lax.rem(j, 2)], NT)
        for u in range(3):
            cols = lanes((3 * j + u) * TQ, TQ)
            sqkv_s[:, cols] = colsum(qkv_s[:, cols].astype(F32))

        @pl.when(j + 2 < n_t)
        def _():
            wq(j + 2).start()

        return carry

    lax.fori_loop(0, n_t, qkv_back, 0)
    ln_bwd(x_s, dm_s, False, g1, x1_s, (0, 1))
    dx_copy = copy(x1_s, dx_o, sem_in.at[0])
    dx_copy.start()

    @pl.when(first == 1)
    def _():
        copy(x1_s, dxs_o.at[c], sem_in.at[7]).start()

    sd_s[6:8, :] = jnp.zeros((2, d), F32)
    for i, (src, dst) in enumerate(((sup_s, sup_o), (sqkv_s, sqkv_o), (sd_s, sd_o))):
        outs.append(copy(src, dst.at[c], sem_out.at[4 + i]))
        outs[-1].start()
    for o in outs:
        o.wait()
    dx_copy.wait()

    zero_put.wait()


def bwd_call(idx, dy_in, ct_all, weights, saved, dx, dx_all, store):
    g1, s1, wqkv, bqkv, wproj, bproj, g2, s2, wup, bup, wdown, bdown = weights
    xs, h1, qkv, mix, x1, h2, pre, lse, act = saved
    n_seq, d = dy_in.shape
    e, f = wqkv.shape[1], wup.shape[1]
    r2 = lambda t: t.reshape(1, -1)
    vm = pl.BlockSpec(memory_space=pltpu.VMEM)
    args = [idx, dy_in, ct_all, xs, qkv, mix, x1, pre, lse, r2(g1), r2(g2), wqkv, wproj.reshape(d, d), wup, wdown]
    alias = [dx, dx_all] + list(store)
    dma = pltpu.SemaphoreType.DMA
    vmem = lambda *s: pltpu.VMEM(s[:-1], s[-1])
    outs = pl.pallas_call(
        bwd_kernel,
        in_specs=[pl.BlockSpec(memory_space=pltpu.SMEM)] + [ANY] * 8 + [vm] * 2 + [ANY] * (4 + len(alias)),
        out_specs=[ANY] * len(alias),
        out_shape=[jax.ShapeDtypeStruct(t.shape, t.dtype) for t in alias],
        input_output_aliases={len(args) + i: i for i in range(len(alias))},
        scratch_shapes=[
            vmem(n_seq, d, BF), vmem(n_seq, d, F32), vmem(2, n_seq, TF, BF), vmem(2, n_seq, n_seq, BF), vmem(4, n_seq, TF, BF), vmem(n_seq, d, BF), vmem(n_seq, d, BF),
            vmem(n_seq, d, BF), vmem(n_seq, e, BF), vmem(n_seq, d, BF), vmem(n_seq, d, BF),
            vmem(n_seq, d, BF), vmem(4, 8, n_seq, F32), vmem(8, n_seq, F32), vmem(384, n_seq, BF), vmem(384, n_seq, BF), vmem(1, f, F32), vmem(1, e, F32), vmem(8, d, F32), vmem(4, 8, d, F32),
            vmem(4, n_seq, TF, F32), vmem(2, TD, e, BF), vmem(d, d, BF), vmem(4, d, TF, BF), vmem(4, TF, d, BF),
            dma((8,)), dma((2,)), dma((4,)), dma((4,)), dma((4,)), dma((4,)), dma((7,)),
        ],
        compiler_params=pltpu.CompilerParams(vmem_limit_bytes=VMEM_LIMIT),
        cost_estimate=pl.CostEstimate(flops=int(36e9), bytes_accessed=int(1.1e8), transcendentals=0),
        name="layer_bwd",
    )(*args, *alias)
    return outs[0], outs[1], tuple(outs[2:])


N_TILE, N_ACC, WT = 12, 3, 1536


def wgrad_kernel(tab, h1, mix, h2, act, dqkv, dmid, dpre, dys, *rest):
    gq, gp, gu, gd, x_s, y_s, xt_s, acc_s, sem_x, sem_y, sem_load, sem_put = rest[4:]
    n = tab[0, 0]
    copy = pltpu.make_async_copy
    two = lambda s: lax.rem(s, 2)
    kinds = ((0, 3, h1, dqkv, gq, False, True, False), (3, 1, mix, dmid, gp, False, False, False),
             (4, 4, h2, dpre, gu, False, True, False), (8, 4, act, dys, gd, True, False, True))

    def by_kind(tile, act_on):
        for base, count, x, y, g, xcol, ycol, grow in kinds:
            @pl.when((tile >= base) & (tile < base + count))
            def _(base=base, x=x, y=y, g=g, xcol=xcol, ycol=ycol, grow=grow):
                at = pl.multiple_of((tile - base) * WT, WT)
                cols = lambda on: pl.ds(at, WT) if on else pl.ds(0, WT)
                act_on(x, y, g.at[cols(grow), cols(ycol)], cols(xcol), cols(ycol))

    def load_xy(s):
        rows = pl.ds(2 * tab[2, s], 2)

        def go(x, y, g, xc, yc):
            copy(x.at[rows, :, xc], x_s.at[two(s)], sem_x.at[two(s)]).start()
            copy(y.at[rows, :, yc], y_s.at[two(s)], sem_y.at[two(s)]).start()

        by_kind(tab[1, s], go)

    slot_of = lambda s: lax.rem(tab[5, s], N_ACC)
    put_done = lambda slot: copy(acc_s.at[slot], gp, sem_put.at[slot]).wait()

    def open_tile(s):
        slot = slot_of(s)

        @pl.when(tab[5, s] >= N_ACC)
        def _():
            put_done(slot)

        @pl.when(tab[3, s] == 1)
        def _():
            by_kind(tab[1, s], lambda x, y, g, xc, yc: copy(g, acc_s.at[slot], sem_load.at[slot]).start())

        @pl.when(tab[3, s] == 0)
        def _():
            acc_s[slot] = jnp.zeros((WT, WT), F32)

    @pl.when(n > 0)
    def _():
        load_xy(0)
        open_tile(0)

    def step(s, carry):
        slot = slot_of(s)

        @pl.when(s + 1 < n)
        def _():
            load_xy(s + 1)

            @pl.when(tab[3, s + 1] < 2)
            def _():
                open_tile(s + 1)

        @pl.when(tab[3, s] == 1)
        def _():
            copy(gp, acc_s.at[slot], sem_load.at[slot]).wait()

        copy(h1.at[pl.ds(0, 2)], x_s.at[two(s)], sem_x.at[two(s)]).wait()
        copy(h1.at[pl.ds(0, 2)], y_s.at[two(s)], sem_y.at[two(s)]).wait()
        x, y = x_s.at[two(s)], y_s.at[two(s)]
        depth = x.shape[0] * x.shape[1]
        for m in range(0, WT, NC):
            xt_s[m // NC] = x[:, :, m:m + NC].reshape(depth, NC).T
        for m in range(0, WT, NC):
            for c in range(0, WT, NC):
                acc_s[slot, m:m + NC, c:c + NC] += mm(xt_s[m // NC], y[:, :, c:c + NC].reshape(depth, NC))

        @pl.when(tab[4, s] == 1)
        def _():
            by_kind(tab[1, s], lambda x, y, g, xc, yc: copy(acc_s.at[slot], g, sem_put.at[slot]).start())

        return carry

    lax.fori_loop(0, n, step, 0)
    for i in range(N_ACC):
        @pl.when(tab[0, 1] > i)
        def _(i=i):
            put_done(lax.rem(tab[0, 1] - 1 - i, N_ACC))


def wgrad_call(tab, saved, store, grads):
    xs, h1, qkv, mix, x1, h2, pre, lse, act = saved
    dpre, dmid, dqkv, dys = store[:4]
    n_seq, d = h1.shape[1:]
    args = [tab, h1, mix, h2, act, dqkv, dmid, dpre, dys]
    dma = pltpu.SemaphoreType.DMA
    return tuple(pl.pallas_call(
        wgrad_kernel,
        in_specs=[pl.BlockSpec(memory_space=pltpu.SMEM)] + [ANY] * (8 + len(grads)),
        out_specs=[ANY] * len(grads),
        out_shape=[jax.ShapeDtypeStruct(g.shape, g.dtype) for g in grads],
        input_output_aliases={len(args) + i: i for i in range(len(grads))},
        scratch_shapes=[
            pltpu.VMEM((2, 2, n_seq, WT), BF), pltpu.VMEM((2, 2, n_seq, WT), BF), pltpu.VMEM((WT // NC, NC, 2 * n_seq), BF),
            pltpu.VMEM((N_ACC, WT, WT), F32), dma((2,)), dma((2,)), dma((N_ACC,)), dma((N_ACC,)),
        ],
        compiler_params=pltpu.CompilerParams(vmem_limit_bytes=VMEM_LIMIT),
        cost_estimate=pl.CostEstimate(flops=int(2e10), bytes_accessed=int(1e8), transcendentals=0),
        name="weight_grad",
    )(*args, *grads))


def fill_table(done, n):
    s = jnp.arange(16, dtype=jnp.int32)
    v = done + s
    pair = v // N_TILE
    head = jnp.where(s < 2, n, 0)
    return jnp.stack([head, v % N_TILE, pair, jnp.where(pair > 0, 1, 0), jnp.ones_like(s), s]).astype(jnp.int32)


def rest_table(done, n_pair):
    total = N_TILE * n_pair
    q, r = done // N_TILE, done % N_TILE
    s = jnp.arange(total + 8, dtype=jnp.int32)
    short, full = jnp.maximum(n_pair - q - 1, 1), jnp.maximum(n_pair - q, 1)
    split = r * (n_pair - q - 1)
    early = s < split
    s2 = s - split
    tile = jnp.where(early, s // short, r + s2 // full)
    within = jnp.where(early, s % short, s2 % full)
    base = jnp.where(early, q + 1, q)
    count = jnp.where(early, short, full)
    mode = jnp.where(within > 0, 2, jnp.where(base > 0, 1, 0))
    start = jnp.where(n_pair - q - 1 > 0, 0, r)
    n = total - done
    head = jnp.where(s == 0, n, jnp.where(s == 1, jnp.where(n > 0, N_TILE - start, 0), 0))
    return jnp.stack([head, tile, base + within, mode, jnp.where(within == count - 1, 1, 0), tile - start]).astype(jnp.int32)


FILL_F, FILL_B = 5, 7


def fresh(shapes):
    return pl.pallas_call(
        lambda *refs: None,
        out_shape=shapes,
        out_specs=[ANY] * len(shapes),
        name="fresh",
    )()


def solution(mesh):
    n_stages = mesh.shape['pp']
    last_stage = n_stages - 1
    fwd_pairs = [(source, source + 1) for source in range(n_stages - 1)]
    bwd_pairs = [(source + 1, source) for source in range(n_stages - 1)]
    act_spec = P(None, 'dp', None, None)
    param_specs = tuple(P(*(('pp',) + (None,) * (rank_n - 1))) for rank_n in PARAM_RANKS)
    grad_specs = tuple(P(*((('dp', 'pp'),) + (None,) * (rank_n - 1))) for rank_n in PARAM_RANKS)

    def stage_body(acts_in, cotangent, *stacked_w):
        weights = tuple(tensor[0] for tensor in stacked_w)
        stage = lax.axis_index('pp')
        n_micro, n_rows, n_seq, d = acts_in.shape
        n_chunk = n_micro * n_rows
        x_all = acts_in.reshape(n_chunk, n_seq, d)
        ct_all = cotangent.reshape(n_chunk, n_seq, d)
        f = 4 * d
        sds = jax.ShapeDtypeStruct
        many = lambda w, t=BF: sds((n_chunk, n_seq, w), t)
        tall = lambda r, w: sds((n_chunk, r, w), F32)
        one = sds((n_seq, d), BF)
        shapes = [many(d), many(d), many(3 * d), many(d), many(d), many(d), many(f, F32), sds((n_chunk, 4, 8, n_seq), F32), many(f),
                  many(f), many(d), many(3 * d), many(d), tall(1, f), tall(1, 3 * d), tall(8, d),
                  many(d), many(d), one, one, one,
                  sds((d, 3 * d), F32), sds((d, d), F32), sds((d, f), F32), sds((f, d), F32)]
        bufs = fresh(shapes)
        saved, store = tuple(bufs[:9]), tuple(bufs[9:16])
        dx_all, y_all, x_in, y, dx = bufs[16:21]
        mats = tuple(bufs[21:])
        n_pair = n_chunk // 2

        def idx_of(c):
            return jnp.stack([jnp.clip(c, 0, n_chunk - 1), stage == 0, stage == last_stage]).astype(jnp.int32)

        def forward(t, x_in, y, y_all, saved):
            c = t - stage
            run = lambda x_in, y, y_all, saved: fwd_call(idx_of(c), x_in, x_all, weights, y, y_all, saved)
            skip = lambda x_in, y, y_all, saved: (y, y_all, saved)
            return lax.cond((c >= 0) & (c < n_chunk), run, skip, x_in, y, y_all, saved)

        def backward(t, dy_in, saved, dx, dx_all, store):
            c = t - (2 * last_stage - stage)
            run = lambda dy_in, saved, dx, dx_all, store: bwd_call(idx_of(c), dy_in, ct_all, weights, saved, dx, dx_all, store)
            skip = lambda dy_in, saved, dx, dx_all, store: (dx, dx_all, store)
            return lax.cond((c >= 0) & (c < n_chunk), run, skip, dy_in, saved, dx, dx_all, store)

        def weight_part(done, ready, limit, saved, store, mats):
            n = jnp.clip(ready - done, 0, limit)
            return done + n, wgrad_call(fill_table(done, n), saved, store, mats)

        def fill(t, state):
            x_in, y, y_all, saved = state
            y, y_all, saved = forward(t, x_in, y, y_all, saved)
            return lax.ppermute(y, 'pp', fwd_pairs), y, y_all, saved

        def steady(t, state):
            x_in, y, y_all, saved, dx, dx_all, store, done, mats = state
            dy_in = lax.ppermute(dx, 'pp', bwd_pairs)
            c = t - stage

            def run(x_in, y, y_all, saved, store, done, mats):
                return fwd_call(idx_of(c), x_in, x_all, weights, y, y_all, saved) + (done, mats)

            def idle(x_in, y, y_all, saved, store, done, mats):
                ready = (t + stage - 2 * last_stage) // 2 * N_TILE
                return (y, y_all, saved) + weight_part(done, ready, FILL_F, saved, store, mats)

            y, y_all, saved, done, mats = lax.cond(c < n_chunk, run, idle, x_in, y, y_all, saved, store, done, mats)
            x_in = lax.ppermute(y, 'pp', fwd_pairs)
            dx, dx_all, store = backward(t, dy_in, saved, dx, dx_all, store)
            return x_in, y, y_all, saved, dx, dx_all, store, done, mats

        def drain(t, state):
            dx, dx_all, store, done, mats = state
            dy_in = lax.ppermute(dx, 'pp', bwd_pairs)
            c = t - (2 * last_stage - stage)

            def run(dy_in, dx, dx_all, store, done, mats):
                return bwd_call(idx_of(c), dy_in, ct_all, weights, saved, dx, dx_all, store) + (done, mats)

            def idle(dy_in, dx, dx_all, store, done, mats):
                return (dx, dx_all, store) + weight_part(done, n_pair * N_TILE, FILL_B, saved, store, mats)

            return lax.cond(c < n_chunk, run, idle, dy_in, dx, dx_all, store, done, mats)

        x_in, y, y_all, saved = lax.fori_loop(0, last_stage, fill, (x_in, y, y_all, saved))
        done = jnp.int32(0)
        x_in, y, y_all, saved, dx, dx_all, store, done, mats = lax.fori_loop(
            last_stage, last_stage + n_chunk, steady, (x_in, y, y_all, saved, dx, dx_all, store, done, mats))
        acts_out = lax.psum(y_all, 'pp')
        dx, dx_all, store, done, mats = lax.fori_loop(
            last_stage + n_chunk, 2 * last_stage + n_chunk, drain, (dx, dx_all, store, done, mats))
        dx_all, acts_out = lax.optimization_barrier((dx_all, acts_out))
        grad_in = lax.psum(dx_all, 'pp')
        g_qkv, g_proj, g_up, g_down = wgrad_call(rest_table(done, n_pair), saved, store, mats)
        sum_up, sum_qkv, sum_d = store[4:]
        vec = jnp.sum(sum_d, axis=0)
        grads = (vec[0], vec[1], g_qkv, jnp.sum(sum_qkv, axis=(0, 1)), g_proj.reshape(stacked_w[4].shape[1:]), vec[4],
                 vec[2], vec[3], g_up, jnp.sum(sum_up, axis=(0, 1)), g_down, vec[5])
        shape4 = acts_in.shape
        return (acts_out.reshape(shape4), grad_in.reshape(shape4)) + tuple(g[None] for g in grads)

    return jax.shard_map(stage_body, mesh=mesh, in_specs=(act_spec, act_spec) + param_specs, out_specs=(act_spec, act_spec) + grad_specs, check_vma=False)
```
